32 devices in a mesh: dp: 8 (over z, core), tensor: 4 (over y, x).
Axes of the slice: x: 2, y: 2, z: 4, core: 2. Of those that a mesh axis runs over, the one named last changes fastest.
Arguments:
- prompt_ids: int32 [4096], P(('dp', 'tensor')), may hold values from 0 to 128255
- prompt_lengths: int32 [8], replicated, may hold values from 1 to 512, as said below
- embed_table: bfloat16 [4096, 128256], P(('dp', 'tensor')), may hold values from -4 to 4
- norm_gain: float32 [4096], replicated, may hold values from 0.5 to 1.5
- w_query: bfloat16 [4096, 4096], P('dp', 'tensor'), may hold values from -3 to 3
- w_key: bfloat16 [4096, 1024], P('dp', 'tensor'), may hold values from -1 to 1
- w_value: bfloat16 [4096, 1024], P('dp', 'tensor'), may hold values from -0.09375 to 0.09375
- w_out: bfloat16 [4096, 4096], P('tensor', 'dp'), may hold values from -0.09375 to 0.09375
Outputs:
- hidden: bfloat16 [4096, 4096], P(('dp', 'tensor'))
- kv_cache: bfloat16 [32, 2, 512, 256], P(('dp', 'tensor'))
The draws below stay inside these ranges and needn't reach their ends.
Inputs may be any that keep to these rules, and one draw needn't show every extreme that they name: `prompt_lengths`: each group's prompt has 1 to 512 live tokens, and some group's has 512.
All inputs are finite; a program needn't handle non-finite values.
Results may differ from the reference program's by a relative error of at most 0.0095.
Values may be sent and summed in bfloat16 or wider, within the bound.
A program may use at most 192 MiB of HBM per device.

```python
import math
import jax
import jax.numpy as jnp
import numpy as np
from jax import lax

D = 4096
HEADS = 32
KVH = 8
HD = 128
VOCAB = 128256
TPG = 4
PROMPT = 512
GROUPS = 8
TOKENS = 4096
N_TENSOR = 4


def draw_prompt_lengths(key, part):
    base = jax.random.randint(jax.random.fold_in(key, 11), (GROUPS,), 1, PROMPT + 1)
    chosen = jax.random.randint(jax.random.fold_in(key, 12), (), 0, GROUPS)
    return jnp.where(jnp.arange(GROUPS) == chosen, PROMPT, base).astype(jnp.int32)


def draw_embed_table(key, part):
    base = jnp.clip(jax.random.normal(jax.random.fold_in(key, 21), (D, VOCAB), jnp.float32), -6.0, 6.0)
    return jnp.clip(0.2 * base, -4.0, 4.0).astype(jnp.bfloat16)


def shared_keys(key):
    base = jax.random.normal(jax.random.fold_in(key, 31), (D, KVH * HD), jnp.float32)
    return jnp.clip(base, -6.0, 6.0) * D ** (-0.5)


def draw_w_key(key, part):
    return jnp.clip(shared_keys(key), -1.0, 1.0).astype(jnp.bfloat16)


def draw_w_query(key, part):
    own = jnp.clip(jax.random.normal(jax.random.fold_in(key, 32), (D, D), jnp.float32), -6.0, 6.0) * D ** (-0.5)
    return jnp.clip(own, -3.0, 3.0).astype(jnp.bfloat16)


def set_ends(values, own_key, smallest, top_value):
    longest = values.shape.index(max(values.shape))
    spots = []
    for shift in (0, 1):
        where = [jax.random.randint(jax.random.fold_in(own_key, axis), (), 0, length) for axis, length in enumerate(values.shape)]
        where[longest] = (where[longest] + shift) % values.shape[longest]
        spots.append(tuple(where))
    return values.at[spots[0]].set(smallest).at[spots[1]].set(top_value)


def level_of(stream_key, shape, pieces, least, top_value):
    gain, own = 1.0, jax.random.fold_in(stream_key, 6)
    for dim, blocks in pieces:
        heights = jnp.exp(jax.random.uniform(jax.random.fold_in(own, dim), (blocks,), jnp.float32, least / len(pieces), top_value / len(pieces)))
        gain = gain * jnp.repeat(heights, shape[dim] // blocks).reshape([-1 if axis == dim else 1 for axis in range(len(shape))])
    return gain


def skewed_wide(stream_key, extent, number_of, slope):
    portions = [min(1 << octave, number_of + 1 - (1 << octave)) * (1 << 20) // math.isqrt((1 << octave) ** slope) + 1 for octave in range((number_of + 1).bit_length()) if 1 << octave <= number_of]
    width = 1 + sum(portions) // (1 << 30)
    grid = np.cumsum(np.array([max(1, weight // width) for weight in portions]))
    lot = jax.random.randint(jax.random.fold_in(stream_key, 1), extent, 0, int(grid[len(portions) - 1]))
    start = jnp.left_shift(1, jnp.searchsorted(jnp.asarray(grid, jnp.int32), lot, side="right").astype(jnp.int32))
    rank = start - 1 + jax.random.randint(jax.random.fold_in(stream_key, 4), extent, 0, 1 << 30) % jnp.minimum(start, number_of + 1 - start)
    return jax.random.permutation(jax.random.fold_in(stream_key, 2), number_of)[rank].astype(jnp.int32)


def scatter_about(stream_key, shape, deviation, bound, split=(), kind=jnp.bfloat16):
    entries = jax.random.normal(stream_key, shape, jnp.float32) * deviation
    if len(split) > 0:
        entries = level_of(stream_key, shape, split, -0.22, 0.18) * entries
    return jnp.clip(entries, min=-bound, max=bound).astype(kind)


def setup_inputs(seed: int = 0) -> dict:
    arg_keys = jax.random.split(jax.random.key(seed), 9)
    return {
        "prompt_ids": set_ends(skewed_wide(arg_keys[0], (TOKENS,), VOCAB, 2), jax.random.fold_in(arg_keys[0], 3), 0, VOCAB - 1).astype(jnp.int32),
        "prompt_lengths": draw_prompt_lengths(jax.random.fold_in(arg_keys[8], 71), 0),
        "embed_table": draw_embed_table(jax.random.fold_in(arg_keys[8], 71), 0),
        "norm_gain": jnp.clip(1.0 + 0.1 * jax.random.normal(arg_keys[3], (D,), jnp.float32), 0.5, 1.5),
        "w_query": draw_w_query(jax.random.fold_in(arg_keys[8], 71), 0),
        "w_key": draw_w_key(jax.random.fold_in(arg_keys[8], 71), 0),
        "w_value": scatter_about(arg_keys[6], (D, KVH * HD), D ** -0.5, 0.09375, ((0, 8), (1, 4))),
        "w_out": scatter_about(arg_keys[7], (D, D), D ** -0.5, 0.09375, ((0, 4), (1, 8))),
    }


norm_eps = 1e-05
rope_theta = 500000.0

def rotate(heads_in, positions):
    half = heads_in.shape[-1] // 2
    freq = rope_theta ** (-2.0 * jnp.arange(half, dtype=jnp.float32) / heads_in.shape[-1])
    angle = positions.astype(jnp.float32)[:, None] * freq[None, :]
    cosine = jnp.cos(angle)[:, None, :]
    sine = jnp.sin(angle)[:, None, :]
    first = heads_in[..., :half]
    second = heads_in[..., half:]
    return jnp.concatenate([first * cosine - second * sine, second * cosine + first * sine], axis=-1)

def attend(query_rot, key_rot, value_rows, length):
    row_count = query_rot.shape[0]
    block = min(512, row_count)
    positions = jnp.arange(row_count, dtype=jnp.int32)
    keys_wide = key_rot.astype(jnp.float32)
    values_wide = value_rows.astype(jnp.float32)

    def one_block(offset):
        queries = lax.dynamic_slice_in_dim(query_rot, offset, block, 0).astype(jnp.float32)
        scores = jnp.einsum('qhgd,khd->hgqk', queries, keys_wide) / jnp.sqrt(jnp.float32(HD))
        query_pos = offset + jnp.arange(block, dtype=jnp.int32)
        allowed = (positions[None, :] <= query_pos[:, None]) & (positions[None, :] < length)
        scores = jnp.where(allowed, scores, -1e+30)
        biggest = lax.optimization_barrier(jnp.max(scores, axis=-1, keepdims=True))
        expd = jnp.exp(scores - biggest)
        weights = (expd / lax.optimization_barrier(jnp.sum(expd, axis=-1, keepdims=True))).astype(jnp.bfloat16)
        result = jnp.einsum('hgqk,khd->qhgd', weights.astype(jnp.float32), values_wide)
        return result.astype(jnp.bfloat16)
    starts = jnp.arange(0, row_count, block, dtype=jnp.int32)
    outs = lax.map(one_block, starts)
    return outs.reshape(row_count, -1)

def layer_group(token_ids, length, embed_table, norm_gain, w_query, w_key, w_value, w_out):
    row_count = token_ids.shape[0]
    tokens_in = jnp.take(embed_table, token_ids, axis=1).T
    wide_in = tokens_in.astype(jnp.float32)
    scale = lax.rsqrt(lax.optimization_barrier(jnp.mean(wide_in * wide_in, axis=1, keepdims=True)) + norm_eps)
    normed = (wide_in * scale * norm_gain.astype(jnp.float32)[None, :]).astype(jnp.bfloat16)
    query = jnp.dot(normed, w_query, preferred_element_type=jnp.float32)
    key_raw = jnp.dot(normed, w_key, preferred_element_type=jnp.float32)
    value_raw = jnp.dot(normed, w_value, preferred_element_type=jnp.float32)
    positions = jnp.arange(row_count, dtype=jnp.int32)
    query_rot = rotate(query.reshape(row_count, HEADS, HD), positions).astype(jnp.bfloat16)
    key_rot = rotate(key_raw.reshape(row_count, KVH, HD), positions).astype(jnp.bfloat16)
    value_rows = value_raw.reshape(row_count, KVH, HD).astype(jnp.bfloat16)
    attended = attend(query_rot.reshape(row_count, KVH, HEADS // KVH, HD), key_rot, value_rows, length)
    blocks = N_TENSOR // TPG
    block_width = D // N_TENSOR
    attended_four = attended.reshape(row_count, blocks, TPG, block_width).astype(jnp.float32)
    out_four = w_out.reshape(blocks, TPG, block_width, D).astype(jnp.float32)
    parts = jnp.einsum('rkmw,kmwd->mrd', attended_four, out_four)
    parts = lax.optimization_barrier(parts.astype(jnp.bfloat16)).astype(jnp.float32)
    hidden = (wide_in + lax.optimization_barrier(jnp.sum(parts, axis=0))).astype(jnp.bfloat16)
    kv_width = KVH * HD // N_TENSOR

    def member_major(table_rows):
        shaped = table_rows.reshape(row_count, blocks, TPG, kv_width)
        return shaped.transpose(2, 0, 1, 3).reshape(TPG, row_count, blocks * kv_width)
    cache = jnp.stack([member_major(key_rot.reshape(row_count, KVH * HD)), member_major(value_rows.reshape(row_count, KVH * HD))], axis=1)
    return (hidden, cache)

def reference(prompt_ids, prompt_lengths, embed_table, norm_gain, w_query, w_key, w_value, w_out):
    grouped_ids = prompt_ids.reshape(GROUPS, PROMPT)

    def one_group(pair):
        return layer_group(pair[0], pair[1], embed_table, norm_gain, w_query, w_key, w_value, w_out)
    hidden, cache = lax.map(one_group, (grouped_ids, prompt_lengths))
    return (hidden.reshape(GROUPS * PROMPT, D), cache.reshape(GROUPS * TPG, 2, PROMPT, KVH * HD // TPG))
```

```python
import functools

import jax
import jax.numpy as jnp
from jax import lax
from jax.experimental import pallas as pl
from jax.experimental.pallas import tpu as pltpu
from jax.sharding import PartitionSpec as P

HEADS = 32
KVH = 8
HD = 128
TPG = 4


norm_eps = 1e-05
rope_theta = 500000.0


def swapped(block, axis, apart):
    count = lax.axis_size(axis)
    route = []
    for low in range(count):
        high = low | 1 << apart
        if high != low and high < count:
            route += [(low, high), (high, low)]
    return lax.ppermute(block, axis, route)


def for_sending(shard):

    def short(part):
        return part.astype(jnp.bfloat16) if part.dtype == jnp.float32 else part

    return jax.tree.map(short, shard)


def rotate(heads_in, positions):
    half = heads_in.shape[-1] // 2
    freq = rope_theta ** (-2.0 * jnp.arange(half, dtype=jnp.float32) / heads_in.shape[-1])
    angle = positions.astype(jnp.float32)[:, None] * freq[None, :]
    cosine = jnp.cos(angle)[:, None, :]
    sine = jnp.sin(angle)[:, None, :]
    first = heads_in[..., :half]
    second = heads_in[..., half:]
    return jnp.concatenate(
        [first * cosine - second * sine, second * cosine + first * sine], axis=-1
    )


def attend(query_rot, key_rot, value_rows, length):
    row_count = query_rot.shape[0]
    block = min(512, row_count)
    positions = jnp.arange(row_count, dtype=jnp.int32)

    def one_block(offset):
        scores = jnp.einsum(
            "qhgd,khd->hgqk", query_rot, key_rot, preferred_element_type=jnp.float32
        ) / jnp.sqrt(jnp.float32(HD))
        query_pos = offset + jnp.arange(block, dtype=jnp.int32)
        allowed = (positions[None, :] <= query_pos[:, None]) & (positions[None, :] < length)
        scores = jnp.where(allowed, scores, -1e30)
        biggest = jnp.max(scores, axis=-1, keepdims=True)
        expd = jnp.exp(scores - biggest)
        weights = (expd / jnp.sum(expd, axis=-1, keepdims=True)).astype(jnp.bfloat16)
        result = jnp.einsum(
            "hgqk,khd->qhgd", weights, value_rows, preferred_element_type=jnp.float32
        )
        return result.astype(jnp.bfloat16)

    starts = jnp.arange(0, row_count, block, dtype=jnp.int32)
    outs = lax.map(one_block, starts)
    return outs.reshape(row_count, -1)


def ordered_pair(mine, theirs, bit_index, axis=0):
    upper_half = lax.axis_index("tensor") >> bit_index & 1 == 1
    first_half = jnp.where(upper_half, theirs, mine)
    second_half = jnp.where(upper_half, mine, theirs)
    return jnp.concatenate([first_half, second_half], axis=axis)


def collect_blocks(shard, swapper):
    stacked = shard[None]
    levels = lax.axis_size("tensor").bit_length() - 1
    for bit_index in range(TPG.bit_length() - 1, levels):
        stacked = ordered_pair(stacked, swapper(stacked, bit_index), bit_index)
    return stacked


def gather_in_group(own_part):
    bits = range(TPG.bit_length() - 1)
    width = own_part.shape[1] // len(bits)
    parts = [own_part[:, i * width : (i + 1) * width] for i in bits]
    axes = (1,) * len(bits)
    parts = [part.reshape(axes + part.shape) for part in parts]
    for step in bits:
        parts = [
            ordered_pair(
                part,
                swapped(part, "tensor", (i + step) % len(bits)),
                (i + step) % len(bits),
                len(bits) - 1 - (i + step) % len(bits),
            )
            for i, part in enumerate(parts)
        ]
    return jnp.concatenate([part.reshape(-1, width) for part in parts], axis=1)


def scatter_in_group(partial_sum):
    bits = range(TPG.bit_length() - 1)
    width = partial_sum.shape[1] // len(bits)
    rows = partial_sum.shape[0] // TPG
    shape = (2,) * len(bits) + (rows, width)
    parts = [partial_sum[:, i * width : (i + 1) * width].reshape(shape) for i in bits]
    for step in bits:
        moved = []
        for i, part in enumerate(parts):
            bit_index = (len(bits) - 1 - i - step) % len(bits)
            axis = len(bits) - 1 - bit_index
            lower = lax.slice_in_dim(part, 0, 1, axis=axis).astype(jnp.bfloat16)
            upper = lax.slice_in_dim(part, 1, 2, axis=axis).astype(jnp.bfloat16)
            upper_half = lax.axis_index("tensor") >> bit_index & 1 == 1
            kept = jnp.where(upper_half, upper, lower)
            given = jnp.where(upper_half, lower, upper)
            arrived = swapped(given, "tensor", bit_index)
            moved.append(kept.astype(jnp.float32) + arrived.astype(jnp.float32))
        parts = moved
    return jnp.concatenate([part.reshape(rows, width) for part in parts], axis=1)


def rms_normed(tokens_in, norm_gain):
    wide_in = tokens_in.astype(jnp.float32)
    scale = lax.rsqrt(jnp.mean(wide_in * wide_in, axis=1, keepdims=True) + norm_eps)
    return (wide_in * scale * norm_gain[None, :]).astype(jnp.bfloat16)


OUT_PARTS = 2
def exchange_kernel(per_target, block_ref, out_ref, own_sem, send_sems, recv_sems):
    width = lax.axis_size("tensor")
    count = lax.axis_size("dp") * width
    me = lax.axis_index("dp") * width + lax.axis_index("tensor")

    def copy_to(apart):
        target = lax.rem(me + apart, count)
        return pltpu.make_async_remote_copy(
            src_ref=block_ref.at[target] if per_target else block_ref.at[0],
            dst_ref=out_ref.at[me],
            send_sem=send_sems.at[apart],
            recv_sem=recv_sems.at[apart],
            device_id={"dp": target // width, "tensor": lax.rem(target, width)},
            device_id_type=pl.DeviceIdType.MESH,
        )

    def start(apart, carry):
        copy_to(apart).start()
        return carry

    def finish(apart, carry):
        copy_to(apart).wait()
        return carry

    own = pltpu.make_async_copy(
        block_ref.at[me] if per_target else block_ref.at[0], out_ref.at[me], own_sem
    )
    own.start()
    lax.fori_loop(1, count, start, 0)
    own.wait()
    lax.fori_loop(1, count, finish, 0)


def exchange(blocks, per_target):
    count = lax.axis_size(("dp", "tensor"))
    return pl.pallas_call(
        functools.partial(exchange_kernel, per_target),
        out_shape=jax.ShapeDtypeStruct((count,) + blocks.shape[1:], blocks.dtype),
        in_specs=[pl.BlockSpec(memory_space=pltpu.VMEM)],
        out_specs=pl.BlockSpec(memory_space=pltpu.VMEM),
        scratch_shapes=[
            pltpu.SemaphoreType.DMA,
            pltpu.SemaphoreType.DMA((count,)),
            pltpu.SemaphoreType.DMA((count,)),
        ],
        compiler_params=pltpu.CompilerParams(
            has_side_effects=True, vmem_limit_bytes=16 << 20
        ),
    )(blocks)


LANES = 128
PIECES = 6


def lookup_kernel(ids_ref, table_ref, out_ref, held, sems):
    columns, vocab = table_ref.shape
    tiles = vocab // LANES
    edges = [i * tiles // PIECES * LANES for i in range(PIECES + 1)]
    copies = [
        pltpu.make_async_copy(
            table_ref.at[:, low:high], held.at[:, low:high], sems.at[i]
        )
        for i, (low, high) in enumerate(zip(edges[:-1], edges[1:]))
    ]
    for copy in copies:
        copy.start()
    for copy in copies:
        copy.wait()
    lane = lax.broadcasted_iota(jnp.int32, (columns, LANES), 1)

    def block(index, carry):
        first = pl.multiple_of(index * LANES, LANES)

        def one(j, total):
            token = ids_ref[first + j]
            start = pl.multiple_of((token >> 7) * LANES, LANES)
            tile = held[:, pl.ds(start, LANES)]
            turned = pltpu.roll(tile, (j - token) & (LANES - 1), 1)
            return jnp.where(lane == j, turned, total)

        total = lax.fori_loop(
            0, LANES, one, jnp.zeros((columns, LANES), out_ref.dtype), unroll=32
        )
        out_ref[pl.ds(first, LANES), :] = total.T
        return carry

    lax.fori_loop(0, out_ref.shape[0] // LANES, block, 0)


def lookup_rows(embed_table, token_ids):
    columns = embed_table.shape[0]
    return pl.pallas_call(
        lookup_kernel,
        out_shape=jax.ShapeDtypeStruct((token_ids.shape[0], columns), embed_table.dtype),
        in_specs=[
            pl.BlockSpec(memory_space=pltpu.SMEM),
            pl.BlockSpec(memory_space=pl.ANY),
        ],
        out_specs=pl.BlockSpec(memory_space=pltpu.VMEM),
        scratch_shapes=[
            pltpu.VMEM(embed_table.shape, embed_table.dtype),
            pltpu.SemaphoreType.DMA((PIECES,)),
        ],
        compiler_params=pltpu.CompilerParams(vmem_limit_bytes=48 << 20),
        cost_estimate=pl.CostEstimate(
            flops=0, bytes_accessed=2 * embed_table.size, transcendentals=0
        ),
    )(token_ids, embed_table)


def general_shards(prompt_ids, prompt_lengths, embed_table, norm_gain, w_query, w_key, w_value, w_out):
    quarter = prompt_ids.shape[0]
    row_count = quarter * TPG
    devices = lax.axis_size(("dp", "tensor"))
    columns = embed_table.shape[0]
    model_width = columns * devices
    group_index = (
        lax.axis_index("dp") * (lax.axis_size("tensor") // TPG) + lax.axis_index("tensor") // TPG
    )
    length = lax.dynamic_slice_in_dim(prompt_lengths, group_index, 1, 0)[0]
    all_ids = exchange(prompt_ids.reshape(1, 1, quarter), False).reshape(-1)
    picked = lookup_rows(embed_table, all_ids)
    outgoing = picked.reshape(devices, quarter, columns)
    arrived = exchange(outgoing, True)
    own_rows = arrived.transpose(1, 0, 2).reshape(quarter, model_width)
    normed = gather_in_group(rms_normed(own_rows, norm_gain))
    query_width = w_query.shape[1]
    key_width = w_key.shape[1]
    packed = jnp.concatenate([w_query, w_key, w_value], axis=1)
    stacked = collect_blocks(
        packed,
        lambda values, bit_index: jax.tree.map(
            lambda part, own: part.astype(own.dtype),
            swapped(for_sending(values), "tensor", bit_index),
            values,
        ),
    )
    projected = jnp.einsum(
        "rd,kdc->rkc",
        normed,
        lax.all_gather(stacked, "dp", axis=1, tiled=True),
        preferred_element_type=jnp.float32,
    )
    blocks = projected.shape[1]
    local_heads = blocks * query_width // HD
    local_kv = blocks * key_width // HD
    positions = jnp.arange(row_count, dtype=jnp.int32)
    query = projected[:, :, :query_width].reshape(row_count, local_heads, HD)
    key_raw = projected[:, :, query_width : query_width + key_width].reshape(
        row_count, local_kv, HD
    )
    value_raw = projected[:, :, query_width + key_width :].reshape(row_count, local_kv, HD)
    query_rot = rotate(query, positions).astype(jnp.bfloat16)
    key_rot = rotate(key_raw, positions).astype(jnp.bfloat16)
    value_rows = value_raw.astype(jnp.bfloat16)
    cache = jnp.stack(
        [key_rot.reshape(row_count, local_kv * HD), value_rows.reshape(row_count, local_kv * HD)],
        axis=0,
    )[None]
    attended = attend(
        query_rot.reshape(row_count, local_kv, HEADS // KVH, HD), key_rot, value_rows, length
    )
    attended = attended.reshape(row_count, blocks, query_width)
    out_blocks = collect_blocks(
        w_out,
        lambda values, bit_index: jax.tree.map(
            lambda part, own: part.astype(own.dtype),
            swapped(for_sending(values), "tensor", bit_index),
            values,
        ),
    )
    width = out_blocks.shape[2] // OUT_PARTS
    reduced = []
    for i in range(OUT_PARTS):
        piece = out_blocks[:, :, i * width : (i + 1) * width]
        partial_sum = jnp.einsum(
            "rkw,kwc->rc",
            attended,
            lax.all_gather(piece, "dp", axis=2, tiled=True),
            preferred_element_type=jnp.float32,
        )
        own_sum = scatter_in_group(partial_sum).reshape(quarter, -1, width)
        attended, own_sum = lax.optimization_barrier((attended, own_sum))
        reduced.append(own_sum)
    running = jnp.concatenate(reduced, axis=2).reshape(quarter, model_width)
    hidden = (own_rows.astype(jnp.float32) + running).astype(jnp.bfloat16)
    return (hidden, cache)


CHUNKS = 6


def chain_kernel(
    lengths_ref, x_ref, gain_ref, cos_ref, sin_ref, wq_ref, wk_ref, wv_ref, wo_ref, wo_low_ref, wo_high_ref,
    hidden_ref, cache_ref,
    feats, mixed_q, mixed_kv, peer_q, peer_k, peer_v, gained, squares, scales, total, passed, inbox,
    out_w, attended, own_part, parts, residual,
    local_sems, w_send, w_recv, x_send, x_recv, sq_send, sq_recv, rs_send, rs_recv,
    o_send, o_recv, d_send, d_recv, r_send, r_recv, p_send, p_recv,
):
    f32, bf16 = jnp.float32, jnp.bfloat16
    dp_size = lax.axis_size("dp")
    members = lax.axis_size("tensor")
    chain = dp_size // 2
    dp = lax.axis_index("dp")
    mine = lax.axis_index("tensor")
    place = dp // 2
    core = lax.rem(dp, 2)
    pool = 2 * members
    self_slot = core * members + mine
    device = dp * members + mine
    lanes = x_ref.shape[1]
    group_rows = feats.shape[1]
    rows = group_rows // members
    shard_rows = wq_ref.shape[0]
    key_width = wk_ref.shape[1]
    heads_kv = key_width // HD
    ratio = HEADS // KVH
    model = lanes * dp_size * members
    columns = wo_ref.shape[1]
    mesh_ids = pl.DeviceIdType.MESH

    def to(dp_index, tensor_index):
        return {"dp": dp_index, "tensor": tensor_index}

    def remote(src, dst, send_sem, recv_sem, dp_index, tensor_index):
        return pltpu.make_async_remote_copy(
            src_ref=src, dst_ref=dst, send_sem=send_sem, recv_sem=recv_sem,
            device_id=to(dp_index, tensor_index), device_id_type=mesh_ids,
        )

    other = dp + 1 - 2 * core

    w_copies = [
        remote(src, dst, w_send.at[i], w_recv.at[i], other, mine)
        for i, (src, dst) in enumerate(((wq_ref, peer_q), (wk_ref, peer_k), (wv_ref, peer_v)))
    ]
    for copy in w_copies:
        copy.start()

    def feature_copy(place_to, slot):
        core_to = slot // members
        first = pl.multiple_of((2 * place_to + core_to) * group_rows, group_rows)
        return remote(
            x_ref.at[pl.ds(first, group_rows), :],
            feats.at[place_to, :, pl.ds(pl.multiple_of(self_slot * lanes, lanes), lanes)],
            x_send.at[place_to * pool + slot],
            x_recv.at[place_to * pool + self_slot],
            2 * place + core_to,
            lax.rem(slot, members),
        )

    def send_features(place_to):
        def one(apart, carry):
            feature_copy(place_to, lax.rem(self_slot + apart, pool)).start()
            return carry

        lax.fori_loop(1, pool, one, 0)

    for step in range(chain - 1):
        right_to = chain - 1 - step
        left_to = step

        @pl.when(right_to > place)
        def _():
            send_features(right_to)

        @pl.when(left_to < place)
        def _():
            send_features(left_to)

    send_features(place)

    def slot_of(back, direction):
        return jnp.where(direction == 0, dp - 2 * back, dp + 2 * back)

    def hop_copy(hop, direction):
        shard = dp - 2 * (hop - 1) if direction == 0 else dp + 2 * (hop - 1)
        target = dp + 2 if direction == 0 else dp - 2
        if hop == 2:
            src = wo_low_ref if direction == 0 else wo_high_ref
        else:
            src = out_w.at[shard]
        return remote(
            src, out_w.at[shard], o_send.at[direction, hop], o_recv.at[direction, hop], target, mine
        )

    def hop_sends(hop, direction):
        if direction == 0:
            return (place - (hop - 1) >= 0) & (place + 1 < chain)
        return (place + (hop - 1) < chain) & (place - 1 >= 0)

    def hop_arrives(hop, direction):
        return place - hop >= 0 if direction == 0 else place + hop < chain

    def hop_wait(hop, direction):
        shard = dp - 2 * hop if direction == 0 else dp + 2 * hop
        remote(
            wo_ref, out_w.at[shard], o_send.at[direction, hop], o_recv.at[direction, hop], other, mine
        ).wait_recv()

    def cross_copy(hop, direction, src):
        shard = dp - 2 * hop if direction == 0 else dp + 2 * hop
        return remote(
            src, out_w.at[shard], d_send.at[direction, hop], d_recv.at[direction, hop], other, mine
        )

    for direction in (0, 1):

        @pl.when(hop_sends(2, direction))
        def _():
            hop_copy(2, direction).start()

    own_out = pltpu.make_async_copy(wo_ref, out_w.at[dp], local_sems.at[0])
    own_out.start()
    cross_copy(0, 0, wo_ref).start()
    near = []
    for direction, ref in ((0, wo_low_ref), (1, wo_high_ref)):
        shard = dp - 2 if direction == 0 else dp + 2

        @pl.when(hop_arrives(1, direction))
        def _():
            pltpu.make_async_copy(ref, out_w.at[shard], local_sems.at[1 + direction]).start()
            cross_copy(1, direction, ref).start()

    def own_features(place_to, carry):
        first = pl.multiple_of((2 * place_to + core) * group_rows, group_rows)
        feats[place_to, :, pl.ds(pl.multiple_of(self_slot * lanes, lanes), lanes)] = x_ref[
            pl.ds(first, group_rows), :
        ]
        return carry

    lax.fori_loop(0, chain, own_features, 0)

    def gain_rows(core_of, q_ref, k_ref, v_ref):
        line = gain_ref[pl.ds(2 * place + core_of, 1), :]
        gained[...] = jnp.broadcast_to(line, (HD, shard_rows)).T
        first = pl.multiple_of(core_of * shard_rows, shard_rows)
        for src, dst, start in ((q_ref, mixed_q, 0), (k_ref, mixed_kv, 0), (v_ref, mixed_kv, key_width)):
            for low in range(0, src.shape[1], HD):
                dst[pl.ds(first, shard_rows), start + low : start + low + HD] = (
                    src[:, low : low + HD].astype(f32) * gained[...]
                ).astype(bf16)

    gain_rows(core, wq_ref, wk_ref, wv_ref)
    for copy in w_copies:
        copy.wait_recv()
    gain_rows(1 - core, peer_q, peer_k, peer_v)

    def square_copy(place_to):
        return remote(
            squares.at[chain + place_to], squares.at[place],
            sq_send.at[place_to], sq_recv.at[place], 2 * place_to + core, mine,
        )

    def features_ready(place_of):
        def one(apart, carry):
            slot = lax.rem(self_slot + apart, pool)
            remote(
                x_ref.at[pl.ds(0, group_rows), :],
                feats.at[place_of, :, pl.ds(pl.multiple_of(slot * lanes, lanes), lanes)],
                x_send.at[place_of * pool + slot],
                x_recv.at[place_of * pool + slot],
                other, mine,
            ).wait_recv()
            return carry

        lax.fori_loop(1, pool, one, 0)
        summed = jnp.zeros((group_rows, lanes), f32)
        for low in range(0, pool * lanes, lanes):
            wide = feats[place_of, :, low : low + lanes].astype(f32)
            summed = summed + wide * wide
        line = jnp.sum(summed.T, axis=0, keepdims=True)
        squares[chain + place_of] = jnp.broadcast_to(line, squares.shape[1:])

    def own_partial(place_of, chunk):
        @pl.when(chunk < 2)
        def _():
            for half in (0, 1):
                first = pl.multiple_of((2 * chunk + half) * rows, rows)
                total[:, half * 2 * key_width : (half + 1) * 2 * key_width] = jnp.dot(
                    feats[place_of, pl.ds(first, rows), :], mixed_kv[...], preferred_element_type=f32
                )

        @pl.when(chunk >= 2)
        def _():
            block = lax.rem(mine + chunk - 1, members)
            total[...] = jnp.dot(
                feats[place_of, pl.ds(pl.multiple_of(block * rows, rows), rows), :],
                mixed_q[...], preferred_element_type=f32,
            )

    def passing_copy(direction, place_to, chunk):
        return remote(
            passed.at[place_to, chunk], inbox.at[direction, place_to, chunk],
            rs_send.at[place_to * CHUNKS + chunk], rs_recv.at[direction, place_to * CHUNKS + chunk],
            dp + 2 - 4 * direction, mine,
        )

    def from_side(direction, place_to, chunk):
        passing_copy(direction, place_to, chunk).wait_recv()
        total[...] += inbox[direction, place_to, chunk].astype(f32)

    lag_right = 2 * jnp.maximum(place - 1, 0)
    lag_left = 2 * jnp.maximum(chain - 2 - place, 0)
    right_count = CHUNKS * (chain - 1 - place)
    left_count = CHUNKS * place

    def pass_step(step, carry):
        direction = lax.rem(step, 2)
        index = step // 2 - jnp.where(direction == 0, lag_right, lag_left)
        count = jnp.where(direction == 0, right_count, left_count)

        @pl.when((index >= 0) & (index < count))
        def _():
            turn = index // CHUNKS
            chunk = lax.rem(index, CHUNKS)
            place_to = jnp.where(direction == 0, chain - 1 - turn, turn)

            @pl.when(chunk == 0)
            def _():
                features_ready(place_to)
                square_copy(place_to).start()

            own_partial(place_to, chunk)
            inner = jnp.where(direction == 0, place > 0, place < chain - 1)

            @pl.when(inner)
            def _():
                from_side(direction, place_to, chunk)

            passed[place_to, chunk] = total[...].astype(bf16)
            passing_copy(direction, place_to, chunk).start()

        return carry

    done = 0
    for hop in range(3, chain):
        until = 2 * CHUNKS * (hop - 2)
        lax.fori_loop(done, until, pass_step, 0)
        done = until
        for direction in (0, 1):

            @pl.when(hop_sends(hop, direction))
            def _():
                hop_wait(hop - 1, direction)
                hop_copy(hop, direction).start()

    lax.fori_loop(done, 2 * (CHUNKS * (chain - 1) + 2 * max(chain - 2, 0)), pass_step, 0)

    def residual_copy(target):
        first = pl.multiple_of(target * rows, rows)
        return remote(
            x_ref.at[pl.ds(first, rows), :],
            residual.at[:, pl.ds(pl.multiple_of(device * lanes, lanes), lanes)],
            r_send.at[target], r_recv.at[device],
            target // members, lax.rem(target, members),
        )

    def start_residual(apart, carry):
        residual_copy(lax.rem(device + apart, dp_size * members)).start()
        return carry

    lax.fori_loop(1, dp_size * members, start_residual, 0)
    residual[:, pl.ds(pl.multiple_of(device * lanes, lanes), lanes)] = x_ref[
        pl.ds(pl.multiple_of(device * rows, rows), rows), :
    ]

    for direction in (0, 1):

        @pl.when(hop_arrives(2, direction))
        def _():
            @pl.when(jnp.logical_not(hop_sends(3, direction)))
            def _():
                hop_wait(2, direction)

            shard = dp - 4 if direction == 0 else dp + 4
            cross_copy(2, direction, out_w.at[shard]).start()

    features_ready(place)
    squares[place] = squares[chain + place]
    for step in range(chain):

        @pl.when(step != place)
        def _():
            remote(
                squares.at[chain + step], squares.at[step],
                sq_send.at[step], sq_recv.at[step], other, mine,
            ).wait_recv()

    summed = squares[0]
    for step in range(1, chain):
        summed = summed + squares[step]
    line = lax.rsqrt(summed[0:1, :] * (1.0 / model) + norm_eps)
    scales[...] = jnp.broadcast_to(line, (HD, group_rows)).T

    def rotated(values, first):
        cosine = cos_ref[pl.ds(first, rows), :]
        sine = sin_ref[pl.ds(first, rows), :]
        return values * cosine + pltpu.roll(values, HD // 2, 1) * sine

    def finish_sum(chunk):
        own_partial(place, chunk)

        @pl.when(place > 0)
        def _():
            from_side(0, place, chunk)

        @pl.when(place < chain - 1)
        def _():
            from_side(1, place, chunk)

    def finish_kv(chunk, carry):
        finish_sum(chunk)
        for half in (0, 1):
            first = pl.multiple_of((2 * chunk + half) * rows, rows)
            scale = scales[pl.ds(first, rows), :]
            for head in range(heads_kv):
                low = half * 2 * key_width + head * HD
                key = rotated(total[:, low : low + HD] * scale, first)
                cache_ref[0, 0, pl.ds(first, rows), head * HD : (head + 1) * HD] = key.astype(bf16)
                value = total[:, low + key_width : low + key_width + HD] * scale
                cache_ref[0, 1, pl.ds(first, rows), head * HD : (head + 1) * HD] = value.astype(bf16)
        return carry

    lax.fori_loop(0, 2, finish_kv, 0)
    length = lengths_ref[dp]

    def attend_block(index):
        block = lax.rem(mine + 1 + index, members)
        first = pl.multiple_of(block * rows, rows)
        finish_sum(index + 2)
        scale = scales[pl.ds(first, rows), :]
        query_pos = first + lax.rem(
            lax.broadcasted_iota(jnp.int32, (ratio * rows, group_rows), 0), rows
        )
        key_pos = lax.broadcasted_iota(jnp.int32, (ratio * rows, group_rows), 1)
        allowed = (key_pos <= query_pos) & (key_pos < length)
        for head in range(heads_kv):
            queries = jnp.concatenate(
                [
                    rotated(total[:, low : low + HD] * scale, first).astype(bf16)
                    for low in range(head * ratio * HD, (head + 1) * ratio * HD, HD)
                ],
                axis=0,
            )
            keys = cache_ref[0, 0, :, head * HD : (head + 1) * HD]
            scores = lax.dot_general(
                queries, keys, (((1,), (1,)), ((), ())), preferred_element_type=f32
            ) * (HD ** -0.5)
            scores = jnp.where(allowed, scores, -1e30)
            expd = jnp.exp(scores - jnp.max(scores, axis=1, keepdims=True))
            weights = (expd / jnp.sum(expd, axis=1, keepdims=True)).astype(bf16)
            result = jnp.dot(
                weights, cache_ref[0, 1, :, head * HD : (head + 1) * HD], preferred_element_type=f32
            )
            for i in range(ratio):
                low = (head * ratio + i) * HD
                attended[index, :, low : low + HD] = result[i * rows : (i + 1) * rows, :].astype(bf16)

    def part_copy(index):
        block = lax.rem(mine + 1 + index, members)
        return remote(
            own_part.at[index], parts.at[mine], p_send.at[index], p_recv.at[mine], dp, block
        )

    def project_block(index):
        def one(shard, carry):
            own_part[index, :, pl.ds(pl.multiple_of(shard * columns, columns), columns)] = jnp.dot(
                attended[index], out_w[shard], preferred_element_type=f32
            ).astype(bf16)
            return carry

        lax.fori_loop(0, dp_size, one, 0)

        @pl.when(index < members - 1)
        def _():
            part_copy(index).start()

    def gather_rest():
        for hop in range(3, chain):
            for direction in (0, 1):

                @pl.when(hop_arrives(hop, direction))
                def _():
                    @pl.when(jnp.logical_not(hop_sends(hop + 1, direction)))
                    def _():
                        hop_wait(hop, direction)

                    shard = dp - 2 * hop if direction == 0 else dp + 2 * hop
                    cross_copy(hop, direction, out_w.at[shard]).start()

        own_out.wait()
        for direction, ref in ((0, wo_low_ref), (1, wo_high_ref)):
            shard = dp - 2 if direction == 0 else dp + 2

            @pl.when(hop_arrives(1, direction))
            def _():
                pltpu.make_async_copy(ref, out_w.at[shard], local_sems.at[1 + direction]).wait()

        for hop in range(chain):
            for direction in (0, 1):
                if hop == 0 and direction == 1:
                    continue

                @pl.when(hop_arrives(hop, direction))
                def _():
                    shard = other - 2 * hop if direction == 0 else other + 2 * hop
                    remote(
                        wo_ref, out_w.at[shard], d_send.at[direction, hop],
                        d_recv.at[direction, hop], other, mine,
                    ).wait_recv()

    at_end = (place == 0) | (place == chain - 1)
    lag_out = jnp.where(at_end, members - 1, 0)

    def finish_step(step, carry):
        @pl.when(step < members)
        def _():
            attend_block(step)

        @pl.when(step == lag_out)
        def _():
            gather_rest()

        @pl.when((step >= lag_out) & (step - lag_out < members))
        def _():
            project_block(step - lag_out)

        return carry

    lax.fori_loop(0, 2 * members - 1, finish_step, 0)

    def residual_wait(apart, carry):
        source = lax.rem(device + apart, dp_size * members)
        remote(
            x_ref.at[pl.ds(0, rows), :],
            residual.at[:, pl.ds(pl.multiple_of(source * lanes, lanes), lanes)],
            r_send.at[source], r_recv.at[source], other, mine,
        ).wait_recv()
        return carry

    lax.fori_loop(1, dp_size * members, residual_wait, 0)
    for apart in range(1, members):
        source = lax.rem(mine + apart, members)
        remote(
            own_part.at[0], parts.at[source], p_send.at[0], p_recv.at[source], dp, mine
        ).wait_recv()

    def add_up(piece, carry):
        span = pl.ds(pl.multiple_of(piece * columns, columns), columns)
        summed = own_part[members - 1, :, span].astype(f32)
        for apart in range(1, members):
            summed = summed + parts[lax.rem(mine + apart, members), :, span].astype(f32)
        hidden_ref[:, span] = (residual[:, span].astype(f32) + summed).astype(bf16)
        return carry

    lax.fori_loop(0, dp_size, add_up, 0)

    for copy in w_copies:
        copy.wait_send()

    def features_sent(place_to, carry):
        def one(apart, inner):
            feature_copy(place_to, lax.rem(self_slot + apart, pool)).wait_send()
            return inner

        return lax.fori_loop(1, pool, one, carry)

    lax.fori_loop(0, chain, features_sent, 0)

    def passes_sent(index, carry):
        place_to = index // CHUNKS

        @pl.when(place_to != place)
        def _():
            passing_copy(0, place_to, lax.rem(index, CHUNKS)).wait_send()

        return carry

    lax.fori_loop(0, chain * CHUNKS, passes_sent, 0)
    for step in range(chain):

        @pl.when(step != place)
        def _():
            square_copy(step).wait_send()

    for hop in range(2, chain):
        for direction in (0, 1):

            @pl.when(hop_sends(hop, direction))
            def _():
                hop_copy(hop, direction).wait_send()

    for hop in range(chain):
        for direction in (0, 1):
            if hop == 0 and direction == 1:
                continue

            @pl.when(hop_arrives(hop, direction))
            def _():
                cross_copy(hop, direction, wo_ref).wait_send()

    def residual_sent(apart, carry):
        residual_copy(lax.rem(device + apart, dp_size * members)).wait_send()
        return carry

    lax.fori_loop(1, dp_size * members, residual_sent, 0)
    for index in range(members - 1):
        part_copy(index).wait_send()


def chain_call(lengths, picked, gain, cosine, sine, w_query, w_key, w_value, w_out, low, high):
    dp_size = lax.axis_size("dp")
    members = lax.axis_size("tensor")
    chain = dp_size // 2
    pool = 2 * members
    tokens, lanes = picked.shape
    group_rows = tokens // dp_size
    rows = group_rows // members
    depth = 2 * w_query.shape[0]
    q_width = w_query.shape[1]
    k_width = w_key.shape[1]
    model = lanes * dp_size * members
    bf16, f32 = jnp.bfloat16, jnp.float32
    dma = pltpu.SemaphoreType.DMA
    vmem = pl.BlockSpec(memory_space=pltpu.VMEM)
    return pl.pallas_call(
        chain_kernel,
        out_shape=(
            jax.ShapeDtypeStruct((rows, model), bf16),
            jax.ShapeDtypeStruct((1, 2, group_rows, k_width), bf16),
        ),
        in_specs=[pl.BlockSpec(memory_space=pltpu.SMEM)] + [vmem] * 10,
        out_specs=(vmem, vmem),
        scratch_shapes=[
            pltpu.VMEM((chain, group_rows, depth), bf16),
            pltpu.VMEM((depth, q_width), bf16),
            pltpu.VMEM((depth, 2 * k_width), bf16),
            pltpu.VMEM(w_query.shape, bf16),
            pltpu.VMEM(w_key.shape, bf16),
            pltpu.VMEM(w_value.shape, bf16),
            pltpu.VMEM((w_query.shape[0], HD), f32),
            pltpu.VMEM((2 * chain, 8, group_rows), f32),
            pltpu.VMEM((group_rows, HD), f32),
            pltpu.VMEM((rows, q_width), f32),
            pltpu.VMEM((chain, CHUNKS, rows, q_width), bf16),
            pltpu.VMEM((2, chain, CHUNKS, rows, q_width), bf16),
            pltpu.VMEM((dp_size,) + w_out.shape, bf16),
            pltpu.VMEM((members, rows, q_width), bf16),
            pltpu.VMEM((members, rows, model), bf16),
            pltpu.VMEM((members, rows, model), bf16),
            pltpu.VMEM((rows, model), bf16),
            dma((3,)), dma((3,)), dma((3,)),
            dma((chain * pool,)), dma((chain * pool,)),
            dma((chain,)), dma((chain,)),
            dma((chain * CHUNKS,)), dma((2, chain * CHUNKS)),
            dma((2, chain + 1)), dma((2, chain + 1)),
            dma((2, chain)), dma((2, chain)),
            dma((dp_size * members,)), dma((dp_size * members,)),
            dma((members,)), dma((members,)),
        ],
        compiler_params=pltpu.CompilerParams(has_side_effects=True, vmem_limit_bytes=62 << 20),
    )(lengths, picked, gain, cosine, sine, w_query, w_key, w_value, w_out, low, high)


def chain_shards(prompt_ids, prompt_lengths, embed_table, norm_gain, w_query, w_key, w_value, w_out):
    quarter = prompt_ids.shape[0]
    dp_size = lax.axis_size("dp")
    group_rows = quarter * lax.axis_size("tensor")
    up = [(i, i + 2) for i in range(dp_size - 2)]
    down = [(i + 2, i) for i in range(dp_size - 2)]
    low = lax.ppermute(w_out, "dp", up)
    high = lax.ppermute(w_out, "dp", down)
    all_ids = exchange(prompt_ids.reshape(1, 1, quarter), False).reshape(-1)
    picked = lookup_rows(embed_table, all_ids)
    half = HD // 2
    freq = rope_theta ** (-2.0 * jnp.arange(half, dtype=jnp.float32) / HD)
    angle = jnp.arange(group_rows, dtype=jnp.float32)[:, None] * freq[None, :]
    cosine = jnp.cos(angle)
    sine = jnp.sin(angle)
    return chain_call(
        prompt_lengths, picked, norm_gain.reshape(dp_size, -1),
        jnp.concatenate([cosine, cosine], axis=1), jnp.concatenate([-sine, sine], axis=1),
        w_query, w_key, w_value, w_out, low, high,
    )


def shards(*args):
    plain = lax.axis_size("tensor") == TPG and lax.axis_size("dp") % 2 == 0
    return (chain_shards if plain else general_shards)(*args)


def solution(mesh):
    in_specs = (
        P(("dp", "tensor")),
        P(),
        P(("dp", "tensor"), None),
        P(),
        P("dp", "tensor"),
        P("dp", "tensor"),
        P("dp", "tensor"),
        P("tensor", "dp"),
    )
    out_specs = (P(("dp", "tensor"), None), P(("dp", "tensor"), None, None, None))
    return jax.shard_map(shards, mesh=mesh, in_specs=in_specs, out_specs=out_specs, check_vma=False)
```

```python
import functools

import jax
import jax.numpy as jnp
import numpy as np
from jax import lax
from jax.experimental import pallas as pl
from jax.experimental.pallas import tpu as pltpu
from jax.sharding import PartitionSpec as P

HEADS = 32
KVH = 8
HD = 128
TPG = 4


norm_eps = 1e-05
rope_theta = 500000.0


def swapped(block, axis, apart):
    count = lax.axis_size(axis)
    route = []
    for low in range(count):
        high = low | 1 << apart
        if high != low and high < count:
            route += [(low, high), (high, low)]
    return lax.ppermute(block, axis, route)


def for_sending(shard):

    def short(part):
        return part.astype(jnp.bfloat16) if part.dtype == jnp.float32 else part

    return jax.tree.map(short, shard)


def rotate(heads_in, positions):
    half = heads_in.shape[-1] // 2
    freq = rope_theta ** (-2.0 * jnp.arange(half, dtype=jnp.float32) / heads_in.shape[-1])
    angle = positions.astype(jnp.float32)[:, None] * freq[None, :]
    cosine = jnp.cos(angle)[:, None, :]
    sine = jnp.sin(angle)[:, None, :]
    first = heads_in[..., :half]
    second = heads_in[..., half:]
    return jnp.concatenate(
        [first * cosine - second * sine, second * cosine + first * sine], axis=-1
    )


def attend(query_rot, key_rot, value_rows, length):
    row_count = query_rot.shape[0]
    block = min(512, row_count)
    positions = jnp.arange(row_count, dtype=jnp.int32)

    def one_block(offset):
        scores = jnp.einsum(
            "qhgd,khd->hgqk", query_rot, key_rot, preferred_element_type=jnp.float32
        ) / jnp.sqrt(jnp.float32(HD))
        query_pos = offset + jnp.arange(block, dtype=jnp.int32)
        allowed = (positions[None, :] <= query_pos[:, None]) & (positions[None, :] < length)
        scores = jnp.where(allowed, scores, -1e30)
        biggest = jnp.max(scores, axis=-1, keepdims=True)
        expd = jnp.exp(scores - biggest)
        weights = (expd / jnp.sum(expd, axis=-1, keepdims=True)).astype(jnp.bfloat16)
        result = jnp.einsum(
            "hgqk,khd->qhgd", weights, value_rows, preferred_element_type=jnp.float32
        )
        return result.astype(jnp.bfloat16)

    starts = jnp.arange(0, row_count, block, dtype=jnp.int32)
    outs = lax.map(one_block, starts)
    return outs.reshape(row_count, -1)


def ordered_pair(mine, theirs, bit_index, axis=0):
    upper_half = lax.axis_index("tensor") >> bit_index & 1 == 1
    first_half = jnp.where(upper_half, theirs, mine)
    second_half = jnp.where(upper_half, mine, theirs)
    return jnp.concatenate([first_half, second_half], axis=axis)


def collect_blocks(shard, swapper):
    stacked = shard[None]
    levels = lax.axis_size("tensor").bit_length() - 1
    for bit_index in range(TPG.bit_length() - 1, levels):
        stacked = ordered_pair(stacked, swapper(stacked, bit_index), bit_index)
    return stacked


def gather_in_group(own_part):
    bits = range(TPG.bit_length() - 1)
    width = own_part.shape[1] // len(bits)
    parts = [own_part[:, i * width : (i + 1) * width] for i in bits]
    axes = (1,) * len(bits)
    parts = [part.reshape(axes + part.shape) for part in parts]
    for step in bits:
        parts = [
            ordered_pair(
                part,
                swapped(part, "tensor", (i + step) % len(bits)),
                (i + step) % len(bits),
                len(bits) - 1 - (i + step) % len(bits),
            )
            for i, part in enumerate(parts)
        ]
    return jnp.concatenate([part.reshape(-1, width) for part in parts], axis=1)


def scatter_in_group(partial_sum):
    bits = range(TPG.bit_length() - 1)
    width = partial_sum.shape[1] // len(bits)
    rows = partial_sum.shape[0] // TPG
    shape = (2,) * len(bits) + (rows, width)
    parts = [partial_sum[:, i * width : (i + 1) * width].reshape(shape) for i in bits]
    for step in bits:
        moved = []
        for i, part in enumerate(parts):
            bit_index = (len(bits) - 1 - i - step) % len(bits)
            axis = len(bits) - 1 - bit_index
            lower = lax.slice_in_dim(part, 0, 1, axis=axis).astype(jnp.bfloat16)
            upper = lax.slice_in_dim(part, 1, 2, axis=axis).astype(jnp.bfloat16)
            upper_half = lax.axis_index("tensor") >> bit_index & 1 == 1
            kept = jnp.where(upper_half, upper, lower)
            given = jnp.where(upper_half, lower, upper)
            arrived = swapped(given, "tensor", bit_index)
            moved.append(kept.astype(jnp.float32) + arrived.astype(jnp.float32))
        parts = moved
    return jnp.concatenate([part.reshape(rows, width) for part in parts], axis=1)


def rms_normed(tokens_in, norm_gain):
    wide_in = tokens_in.astype(jnp.float32)
    scale = lax.rsqrt(jnp.mean(wide_in * wide_in, axis=1, keepdims=True) + norm_eps)
    return (wide_in * scale * norm_gain[None, :]).astype(jnp.bfloat16)


OUT_PARTS = 2
def exchange_kernel(per_target, block_ref, out_ref, own_sem, send_sems, recv_sems):
    width = lax.axis_size("tensor")
    count = lax.axis_size("dp") * width
    me = lax.axis_index("dp") * width + lax.axis_index("tensor")

    def copy_to(apart):
        target = lax.rem(me + apart, count)
        return pltpu.make_async_remote_copy(
            src_ref=block_ref.at[target] if per_target else block_ref.at[0],
            dst_ref=out_ref.at[me],
            send_sem=send_sems.at[apart],
            recv_sem=recv_sems.at[apart],
            device_id={"dp": target // width, "tensor": lax.rem(target, width)},
            device_id_type=pl.DeviceIdType.MESH,
        )

    def start(apart, carry):
        copy_to(apart).start()
        return carry

    def finish(apart, carry):
        copy_to(apart).wait()
        return carry

    own = pltpu.make_async_copy(
        block_ref.at[me] if per_target else block_ref.at[0], out_ref.at[me], own_sem
    )
    own.start()
    lax.fori_loop(1, count, start, 0)
    own.wait()
    lax.fori_loop(1, count, finish, 0)


def exchange(blocks, per_target):
    count = lax.axis_size(("dp", "tensor"))
    return pl.pallas_call(
        functools.partial(exchange_kernel, per_target),
        out_shape=jax.ShapeDtypeStruct((count,) + blocks.shape[1:], blocks.dtype),
        in_specs=[pl.BlockSpec(memory_space=pltpu.VMEM)],
        out_specs=pl.BlockSpec(memory_space=pltpu.VMEM),
        scratch_shapes=[
            pltpu.SemaphoreType.DMA,
            pltpu.SemaphoreType.DMA((count,)),
            pltpu.SemaphoreType.DMA((count,)),
        ],
        compiler_params=pltpu.CompilerParams(
            has_side_effects=True, vmem_limit_bytes=16 << 20
        ),
    )(blocks)


LANES = 128
PIECES = 6


def lookup_kernel(ids_ref, table_ref, out_ref, held, sems):
    columns, vocab = table_ref.shape
    tiles = vocab // LANES
    edges = [i * tiles // PIECES * LANES for i in range(PIECES + 1)]
    copies = [
        pltpu.make_async_copy(
            table_ref.at[:, low:high], held.at[:, low:high], sems.at[i]
        )
        for i, (low, high) in enumerate(zip(edges[:-1], edges[1:]))
    ]
    for copy in copies:
        copy.start()
    for copy in copies:
        copy.wait()
    lane = lax.broadcasted_iota(jnp.int32, (columns, LANES), 1)

    def block(index, carry):
        first = pl.multiple_of(index * LANES, LANES)

        def one(j, total):
            token = ids_ref[first + j]
            start = pl.multiple_of((token >> 7) * LANES, LANES)
            tile = held[:, pl.ds(start, LANES)]
            turned = pltpu.roll(tile, (j - token) & (LANES - 1), 1)
            return jnp.where(lane == j, turned, total)

        total = lax.fori_loop(
            0, LANES, one, jnp.zeros((columns, LANES), out_ref.dtype), unroll=32
        )
        out_ref[pl.ds(first, LANES), :] = total.T
        return carry

    lax.fori_loop(0, out_ref.shape[0] // LANES, block, 0)


def lookup_rows(embed_table, token_ids):
    columns = embed_table.shape[0]
    return pl.pallas_call(
        lookup_kernel,
        out_shape=jax.ShapeDtypeStruct((token_ids.shape[0], columns), embed_table.dtype),
        in_specs=[
            pl.BlockSpec(memory_space=pltpu.SMEM),
            pl.BlockSpec(memory_space=pl.ANY),
        ],
        out_specs=pl.BlockSpec(memory_space=pltpu.VMEM),
        scratch_shapes=[
            pltpu.VMEM(embed_table.shape, embed_table.dtype),
            pltpu.SemaphoreType.DMA((PIECES,)),
        ],
        compiler_params=pltpu.CompilerParams(vmem_limit_bytes=48 << 20),
        cost_estimate=pl.CostEstimate(
            flops=0, bytes_accessed=2 * embed_table.size, transcendentals=0
        ),
    )(token_ids, embed_table)


def general_shards(prompt_ids, prompt_lengths, embed_table, norm_gain, w_query, w_key, w_value, w_out):
    quarter = prompt_ids.shape[0]
    row_count = quarter * TPG
    devices = lax.axis_size(("dp", "tensor"))
    columns = embed_table.shape[0]
    model_width = columns * devices
    group_index = (
        lax.axis_index("dp") * (lax.axis_size("tensor") // TPG) + lax.axis_index("tensor") // TPG
    )
    length = lax.dynamic_slice_in_dim(prompt_lengths, group_index, 1, 0)[0]
    all_ids = exchange(prompt_ids.reshape(1, 1, quarter), False).reshape(-1)
    picked = lookup_rows(embed_table, all_ids)
    outgoing = picked.reshape(devices, quarter, columns)
    arrived = exchange(outgoing, True)
    own_rows = arrived.transpose(1, 0, 2).reshape(quarter, model_width)
    normed = gather_in_group(rms_normed(own_rows, norm_gain))
    query_width = w_query.shape[1]
    key_width = w_key.shape[1]
    packed = jnp.concatenate([w_query, w_key, w_value], axis=1)
    stacked = collect_blocks(
        packed,
        lambda values, bit_index: jax.tree.map(
            lambda part, own: part.astype(own.dtype),
            swapped(for_sending(values), "tensor", bit_index),
            values,
        ),
    )
    projected = jnp.einsum(
        "rd,kdc->rkc",
        normed,
        lax.all_gather(stacked, "dp", axis=1, tiled=True),
        preferred_element_type=jnp.float32,
    )
    blocks = projected.shape[1]
    local_heads = blocks * query_width // HD
    local_kv = blocks * key_width // HD
    positions = jnp.arange(row_count, dtype=jnp.int32)
    query = projected[:, :, :query_width].reshape(row_count, local_heads, HD)
    key_raw = projected[:, :, query_width : query_width + key_width].reshape(
        row_count, local_kv, HD
    )
    value_raw = projected[:, :, query_width + key_width :].reshape(row_count, local_kv, HD)
    query_rot = rotate(query, positions).astype(jnp.bfloat16)
    key_rot = rotate(key_raw, positions).astype(jnp.bfloat16)
    value_rows = value_raw.astype(jnp.bfloat16)
    cache = jnp.stack(
        [key_rot.reshape(row_count, local_kv * HD), value_rows.reshape(row_count, local_kv * HD)],
        axis=0,
    )[None]
    attended = attend(
        query_rot.reshape(row_count, local_kv, HEADS // KVH, HD), key_rot, value_rows, length
    )
    attended = attended.reshape(row_count, blocks, query_width)
    out_blocks = collect_blocks(
        w_out,
        lambda values, bit_index: jax.tree.map(
            lambda part, own: part.astype(own.dtype),
            swapped(for_sending(values), "tensor", bit_index),
            values,
        ),
    )
    width = out_blocks.shape[2] // OUT_PARTS
    reduced = []
    for i in range(OUT_PARTS):
        piece = out_blocks[:, :, i * width : (i + 1) * width]
        partial_sum = jnp.einsum(
            "rkw,kwc->rc",
            attended,
            lax.all_gather(piece, "dp", axis=2, tiled=True),
            preferred_element_type=jnp.float32,
        )
        own_sum = scatter_in_group(partial_sum).reshape(quarter, -1, width)
        attended, own_sum = lax.optimization_barrier((attended, own_sum))
        reduced.append(own_sum)
    running = jnp.concatenate(reduced, axis=2).reshape(quarter, model_width)
    hidden = (own_rows.astype(jnp.float32) + running).astype(jnp.bfloat16)
    return (hidden, cache)


CHUNKS = 6
TURN = 16


def chain_kernel(
    lengths_ref, ids_ref, table_ref, gain_ref, cos_ref, sin_ref, wq_ref, wk_ref, wv_ref, wo_ref,
    hidden_ref, cache_ref, out_w,
    held, ids_all, ids_scalar, x_ref,
    feats, mixed_q, mixed_kv, peer_q, peer_k, peer_v, gained, squares, scales, total, passed, inbox, residual,
    table_sems, ids_sems, i_send, i_recv,
    w_send, w_recv, x_send, x_recv, sq_send, sq_recv, rs_send, rs_recv,
    o_send, o_recv, d_send, d_recv, r_send, r_recv, p_send, p_recv, load_sems,
):
    f32, bf16 = jnp.float32, jnp.bfloat16
    dp_size = lax.axis_size("dp")
    members = lax.axis_size("tensor")
    chain = dp_size // 2
    dp = lax.axis_index("dp")
    mine = lax.axis_index("tensor")
    place = dp // 2
    core = lax.rem(dp, 2)
    pool = 2 * members
    self_slot = core * members + mine
    device = dp * members + mine
    lanes = x_ref.shape[1]
    group_rows = feats.shape[1]
    rows = group_rows // members
    shard_rows = wq_ref.shape[0]
    key_width = wk_ref.shape[1]
    heads_kv = key_width // HD
    ratio = HEADS // KVH
    model = lanes * dp_size * members
    depth, columns = wo_ref.shape
    devices = dp_size * members
    q_width = wq_ref.shape[1]
    at_shards = 0
    across = columns // LANES
    shard_tiles = depth // LANES * across
    q_tiles = q_width // LANES
    model_tiles = model // LANES
    at_attended = at_shards + dp_size * shard_tiles
    at_own = at_attended + members * q_tiles
    at_parts = at_own + members * model_tiles
    mesh_ids = pl.DeviceIdType.MESH

    def to(dp_index, tensor_index):
        return {"dp": dp_index, "tensor": tensor_index}

    def remote(src, dst, send_sem, recv_sem, dp_index, tensor_index):
        return pltpu.make_async_remote_copy(
            src_ref=src, dst_ref=dst, send_sem=send_sem, recv_sem=recv_sem,
            device_id=to(dp_index, tensor_index), device_id_type=mesh_ids,
        )

    other = dp + 1 - 2 * core

    w_copies = [
        remote(src, dst, w_send.at[i], w_recv.at[i], other, mine)
        for i, (src, dst) in enumerate(((wq_ref, peer_q), (wk_ref, peer_k), (wv_ref, peer_v)))
    ]
    for copy in w_copies:
        copy.start()

    def ids_copy(target):
        return remote(
            ids_ref.at[0], ids_all.at[device], i_send.at[target], i_recv.at[device],
            target // members, lax.rem(target, members),
        )

    def start_ids(apart, carry):
        ids_copy(lax.rem(device + apart, devices)).start()
        return carry

    lax.fori_loop(1, devices, start_ids, 0)
    ids_all[device] = ids_ref[0]

    def start_tile(tile, carry):
        pltpu.make_async_copy(
            table_ref.at[:, pl.ds(pl.multiple_of(tile * LANES, LANES), LANES)], held.at[tile], table_sems.at[0]
        ).start()
        return carry

    lax.fori_loop(0, held.shape[0], start_tile, 0, unroll=6)

    def wait_ids(apart, carry):
        source = lax.rem(device + apart, devices)
        remote(
            ids_ref.at[0], ids_all.at[source], i_send.at[source], i_recv.at[source], other, mine
        ).wait_recv()
        return carry

    lax.fori_loop(1, devices, wait_ids, 0)
    ids_copy_in = pltpu.make_async_copy(ids_all, ids_scalar, ids_sems.at[0])
    ids_copy_in.start()

    def feature_copy(place_to, slot):
        core_to = slot // members
        first = pl.multiple_of((2 * place_to + core_to) * group_rows, group_rows)
        return remote(
            x_ref.at[pl.ds(first, group_rows), :],
            feats.at[place_to, :, pl.ds(pl.multiple_of(self_slot * lanes, lanes), lanes)],
            x_send.at[place_to * pool + slot],
            x_recv.at[place_to * pool + self_slot],
            2 * place + core_to,
            lax.rem(slot, members),
        )

    lane = lax.broadcasted_iota(jnp.int32, (lanes, LANES), 1)
    turn_row = lax.broadcasted_iota(jnp.int32, (TURN, 2 * LANES), 0)
    turn_spot = lax.broadcasted_iota(jnp.int32, (TURN, 2 * LANES), 1)
    low_half = lax.broadcasted_iota(jnp.int32, (TURN, LANES), 0) % 4 < 2

    def tile_of(token):
        return held[token // LANES]

    def lookup_pair(pair, carry):
        first = pl.multiple_of(pair * 2 * LANES, LANES)
        second = pl.multiple_of(first + LANES, LANES)

        def turn(step, rolled):
            picked = jnp.zeros((TURN, 2 * LANES), f32)
            for four in range(0, TURN, 4):
                tokens = [ids_scalar[2 * pair + 1, 0, step * TURN + four + i] for i in range(4)]
                tiles_of = [tile_of(token) for token in tokens]
                where = jnp.full((TURN, 2 * LANES), -1, jnp.int32)
                for i, token in enumerate(tokens):
                    where = jnp.where(
                        turn_row == four + i, (token & (LANES - 1)) + (i % 2) * LANES, where
                    )
                chosen = jnp.where(where == turn_spot, 1.0, 0.0).astype(bf16)
                stacked = jnp.concatenate(
                    [jnp.concatenate(tiles_of[:2], axis=1), jnp.concatenate(tiles_of[2:], axis=1)],
                    axis=0,
                )
                picked = picked + lax.dot_general(
                    chosen, stacked, (((1,), (1,)), ((), ())), preferred_element_type=f32
                )
            x_ref[pl.ds(pl.multiple_of(second + step * TURN, TURN), TURN), :] = jnp.where(
                low_half, picked[:, :LANES], picked[:, LANES:]
            ).astype(bf16)
            for i in range(TURN):
                j = step * TURN + i
                token = ids_scalar[2 * pair, 0, j]
                turned = pltpu.roll(tile_of(token), (j - token) & (LANES - 1), 1)
                rolled = jnp.where(lane == j, turned, rolled)
            return rolled

        rolled = lax.fori_loop(0, LANES // TURN, turn, jnp.zeros((lanes, LANES), bf16), unroll=4)
        x_ref[pl.ds(first, LANES), :] = rolled.T
        return carry

    def order_of(index):
        found, picked = jnp.int32(0), jnp.int32(0)
        for step in range(chain - 1):
            for candidate, valid in (
                (chain - 1 - step, (chain - 1 - step > place).astype(jnp.int32)),
                (step, (step < place).astype(jnp.int32)),
            ):
                picked = picked + jnp.where((valid == 1) & (found == index), candidate, 0)
                found = found + valid
        return picked + jnp.where(index == chain - 1, place, 0)

    pairs = group_rows // (2 * LANES)

    def look_up(index, carry):
        place_to = order_of(index)

        def send(core_to):
            def one(apart, inner):
                slot = core_to * members + lax.rem(mine + apart, members)

                @pl.when(slot != self_slot)
                def _():
                    feature_copy(place_to, slot).start()

                return inner

            lax.fori_loop(1, members + 1, one, 0)

        def one_group(core_to, inner):
            group = 2 * place_to + core_to
            lax.fori_loop(group * pairs, (group + 1) * pairs, lookup_pair, 0)

            @pl.when(index < chain - 1)
            def _():
                send(core_to)

            @pl.when((index == chain - 1) & (core_to == 1))
            def _():
                send(0)
                send(1)

            @pl.when(core_to == core)
            def _():
                first = pl.multiple_of(group * group_rows, group_rows)
                feats[place_to, :, pl.ds(pl.multiple_of(self_slot * lanes, lanes), lanes)] = x_ref[
                    pl.ds(first, group_rows), :
                ]

            return inner

        lax.fori_loop(0, 2, one_group, 0)
        return carry

    def hop_copy(hop, direction):
        shard = dp - 2 * (hop - 1) if direction == 0 else dp + 2 * (hop - 1)
        target = dp + 2 if direction == 0 else dp - 2
        src = wo_ref if hop == 1 else out_w.at[shard]
        return remote(
            src, out_w.at[shard], o_send.at[direction, hop], o_recv.at[direction, hop], target, mine
        )

    def hop_sends(hop, direction):
        if direction == 0:
            return (place - (hop - 1) >= 0) & (place + 1 < chain)
        return (place + (hop - 1) < chain) & (place - 1 >= 0)

    def hop_arrives(hop, direction):
        return place - hop >= 0 if direction == 0 else place + hop < chain

    def hop_wait(hop, direction):
        shard = dp - 2 * hop if direction == 0 else dp + 2 * hop
        remote(
            wo_ref, out_w.at[shard], o_send.at[direction, hop], o_recv.at[direction, hop], other, mine
        ).wait_recv()

    def cross_copy(hop, direction, src):
        shard = dp - 2 * hop if direction == 0 else dp + 2 * hop
        return remote(
            src, out_w.at[shard], d_send.at[direction, hop], d_recv.at[direction, hop], other, mine
        )

    for direction in (0, 1):

        @pl.when(hop_sends(1, direction))
        def _():
            hop_copy(1, direction).start()

    cross_copy(0, 0, wo_ref).start()

    def gain_rows(core_of, q_ref, k_ref, v_ref):
        line = gain_ref[pl.ds(2 * place + core_of, 1), :]
        gained[...] = jnp.broadcast_to(line, (HD, shard_rows)).T
        first = pl.multiple_of(core_of * shard_rows, shard_rows)
        for src, dst, start in ((q_ref, mixed_q, 0), (k_ref, mixed_kv, 0), (v_ref, mixed_kv, key_width)):
            for low in range(0, src.shape[1], HD):
                dst[pl.ds(first, shard_rows), start + low : start + low + HD] = (
                    src[:, low : low + HD].astype(f32) * gained[...]
                ).astype(bf16)

    gain_rows(core, wq_ref, wk_ref, wv_ref)
    for copy in w_copies:
        copy.wait_recv()
    gain_rows(1 - core, peer_q, peer_k, peer_v)
    ids_copy_in.wait()
    pltpu.make_async_copy(held, held, table_sems.at[0]).wait()

    def square_copy(place_to):
        return remote(
            squares.at[chain + place_to], squares.at[place],
            sq_send.at[place_to], sq_recv.at[place], 2 * place_to + core, mine,
        )

    def features_ready(place_of):
        def one(apart, carry):
            slot = lax.rem(self_slot + apart, pool)
            remote(
                x_ref.at[pl.ds(0, group_rows), :],
                feats.at[place_of, :, pl.ds(pl.multiple_of(slot * lanes, lanes), lanes)],
                x_send.at[place_of * pool + slot],
                x_recv.at[place_of * pool + slot],
                other, mine,
            ).wait_recv()
            return carry

        lax.fori_loop(1, pool, one, 0)
        summed = jnp.zeros((group_rows, lanes), f32)
        for low in range(0, pool * lanes, lanes):
            wide = feats[place_of, :, low : low + lanes].astype(f32)
            summed = summed + wide * wide
        line = jnp.sum(summed.T, axis=0, keepdims=True)
        squares[chain + place_of] = jnp.broadcast_to(line, squares.shape[1:])

    def own_partial(place_of, chunk):
        @pl.when(chunk < 2)
        def _():
            for half in (0, 1):
                first = pl.multiple_of((2 * chunk + half) * rows, rows)
                total[:, half * 2 * key_width : (half + 1) * 2 * key_width] = jnp.dot(
                    feats[place_of, pl.ds(first, rows), :], mixed_kv[...], preferred_element_type=f32
                )

        @pl.when(chunk >= 2)
        def _():
            block = lax.rem(mine + chunk - 1, members)
            total[...] = jnp.dot(
                feats[place_of, pl.ds(pl.multiple_of(block * rows, rows), rows), :],
                mixed_q[...], preferred_element_type=f32,
            )

    def out_slot(place_to):
        return place_to - (place_to > place).astype(jnp.int32)

    def passing_copy(direction, place_to, chunk):
        return remote(
            passed.at[out_slot(place_to), chunk], inbox.at[place_to + 1 - direction, chunk],
            rs_send.at[place_to * CHUNKS + chunk], rs_recv.at[direction, place_to * CHUNKS + chunk],
            dp + 2 - 4 * direction, mine,
        )

    def from_side(direction, place_to, chunk):
        remote(
            passed.at[0, chunk], inbox.at[place_to + 1 - direction, chunk],
            rs_send.at[0], rs_recv.at[direction, place_to * CHUNKS + chunk], other, mine,
        ).wait_recv()
        total[...] += inbox[place_to + 1 - direction, chunk].astype(f32)

    lag_right = 2 * jnp.maximum(place - 1, 0)
    lag_left = 2 * jnp.maximum(chain - 2 - place, 0)
    right_count = CHUNKS * (chain - 1 - place)
    left_count = CHUNKS * place

    def pass_step(step, carry):
        direction = lax.rem(step, 2)
        index = step // 2 - jnp.where(direction == 0, lag_right, lag_left)
        count = jnp.where(direction == 0, right_count, left_count)

        @pl.when((index >= 0) & (index < count))
        def _():
            turn = index // CHUNKS
            chunk = lax.rem(index, CHUNKS)
            place_to = jnp.where(direction == 0, chain - 1 - turn, turn)

            @pl.when(chunk == 0)
            def _():
                features_ready(place_to)
                square_copy(place_to).start()

            own_partial(place_to, chunk)
            inner = jnp.where(direction == 0, place > 0, place < chain - 1)

            @pl.when(inner)
            def _():
                from_side(direction, place_to, chunk)

            passed[out_slot(place_to), chunk] = total[...].astype(bf16)
            passing_copy(direction, place_to, chunk).start()

        return carry

    at_end = (place == 0) | (place == chain - 1)

    def looked_up(turn):
        early = jnp.minimum(2 + turn // CHUNKS, chain)
        return jnp.where(turn < 0, 0, jnp.where(at_end, early, chain))

    def stream_turn(turn, carry):
        lax.fori_loop(looked_up(turn - 1), looked_up(turn), look_up, 0)
        for hop in range(2, chain):
            for direction in (0, 1):

                @pl.when((turn == CHUNKS * (hop - 2)) & hop_sends(hop, direction))
                def _():
                    hop_wait(hop - 1, direction)
                    hop_copy(hop, direction).start()

        return lax.fori_loop(2 * turn, 2 * turn + 2, pass_step, carry)

    lax.fori_loop(0, CHUNKS * (chain - 1) + 2 * max(chain - 2, 0), stream_turn, 0)

    def residual_copy(target):
        first = pl.multiple_of(target * rows, rows)
        return remote(
            x_ref.at[pl.ds(first, rows), :],
            residual.at[:, pl.ds(pl.multiple_of(device * lanes, lanes), lanes)],
            r_send.at[target], r_recv.at[device],
            target // members, lax.rem(target, members),
        )

    def start_residual(apart, carry):
        residual_copy(lax.rem(device + apart, devices)).start()
        return carry

    lax.fori_loop(1, devices, start_residual, 0)
    residual[:, pl.ds(pl.multiple_of(device * lanes, lanes), lanes)] = x_ref[
        pl.ds(pl.multiple_of(device * rows, rows), rows), :
    ]

    def to_other_core(hop):
        for direction in (0, 1):

            @pl.when(hop_arrives(hop, direction))
            def _():
                @pl.when(jnp.logical_not(hop_sends(hop + 1, direction)))
                def _():
                    hop_wait(hop, direction)

                shard = dp - 2 * hop if direction == 0 else dp + 2 * hop
                cross_copy(hop, direction, out_w.at[shard]).start()

    for hop in range(1, min(chain, 3)):
        to_other_core(hop)

    features_ready(place)
    squares[place] = squares[chain + place]
    for step in range(chain):

        @pl.when(step != place)
        def _():
            remote(
                squares.at[chain + step], squares.at[step],
                sq_send.at[step], sq_recv.at[step], other, mine,
            ).wait_recv()

    summed = squares[0]
    for step in range(1, chain):
        summed = summed + squares[step]
    line = lax.rsqrt(summed[0:1, :] * (1.0 / model) + norm_eps)
    scales[...] = jnp.broadcast_to(line, (HD, group_rows)).T

    def rotated(values, first):
        cosine = cos_ref[pl.ds(first, rows), :]
        sine = sin_ref[pl.ds(first, rows), :]
        return values * cosine + pltpu.roll(values, HD // 2, 1) * sine

    def finish_sum(chunk):
        own_partial(place, chunk)

        @pl.when(place > 0)
        def _():
            from_side(0, place, chunk)

        @pl.when(place < chain - 1)
        def _():
            from_side(1, place, chunk)

    def finish_kv(chunk, carry):
        finish_sum(chunk)
        for half in (0, 1):
            first = pl.multiple_of((2 * chunk + half) * rows, rows)
            scale = scales[pl.ds(first, rows), :]
            for head in range(heads_kv):
                low = half * 2 * key_width + head * HD
                key = rotated(total[:, low : low + HD] * scale, first)
                cache_ref[0, 0, pl.ds(first, rows), head * HD : (head + 1) * HD] = key.astype(bf16)
                value = total[:, low + key_width : low + key_width + HD] * scale
                cache_ref[0, 1, pl.ds(first, rows), head * HD : (head + 1) * HD] = value.astype(bf16)
        return carry

    lax.fori_loop(0, 2, finish_kv, 0)
    length = lengths_ref[dp]

    def attend_block(index):
        block = lax.rem(mine + 1 + index, members)
        first = pl.multiple_of(block * rows, rows)
        finish_sum(index + 2)
        scale = scales[pl.ds(first, rows), :]
        query_pos = first + lax.rem(
            lax.broadcasted_iota(jnp.int32, (ratio * rows, group_rows), 0), rows
        )
        key_pos = lax.broadcasted_iota(jnp.int32, (ratio * rows, group_rows), 1)
        allowed = (key_pos <= query_pos) & (key_pos < length)
        for head in range(heads_kv):
            queries = jnp.concatenate(
                [
                    rotated(total[:, low : low + HD] * scale, first).astype(bf16)
                    for low in range(head * ratio * HD, (head + 1) * ratio * HD, HD)
                ],
                axis=0,
            )
            keys = cache_ref[0, 0, :, head * HD : (head + 1) * HD]
            scores = lax.dot_general(
                queries, keys, (((1,), (1,)), ((), ())), preferred_element_type=f32
            ) * (HD ** -0.5)
            scores = jnp.where(allowed, scores, -1e30)
            expd = jnp.exp(scores - jnp.max(scores, axis=1, keepdims=True))
            weights = (expd / jnp.sum(expd, axis=1, keepdims=True)).astype(bf16)
            result = jnp.dot(
                weights, cache_ref[0, 1, :, head * HD : (head + 1) * HD], preferred_element_type=f32
            )
            for i in range(ratio):
                low = (head * ratio + i) * HD
                held[at_attended + index * q_tiles + head * ratio + i] = result[i * rows : (i + 1) * rows, :].astype(bf16)

    def part_copy(index):
        block = lax.rem(mine + 1 + index, members)
        return remote(
            held.at[pl.ds(at_own + index * model_tiles, model_tiles)],
            held.at[pl.ds(at_parts + mine * model_tiles, model_tiles)], p_send.at[index], p_recv.at[mine], dp, block
        )

    def project_block(index):
        def one(shard, carry):
            base = at_shards + shard * shard_tiles
            weights = jnp.concatenate(
                [
                    jnp.concatenate([held[base + i * across + q] for q in range(across)], axis=1)
                    for i in range(depth // LANES)
                ],
                axis=0,
            )
            heads = jnp.concatenate(
                [held[at_attended + index * q_tiles + head] for head in range(q_tiles)], axis=1
            )
            result = jnp.dot(heads, weights, preferred_element_type=f32).astype(bf16)
            for q in range(across):
                held[at_own + index * model_tiles + shard * across + q] = result[
                    :, q * LANES : (q + 1) * LANES
                ]
            return carry

        lax.fori_loop(0, dp_size, one, 0)

        @pl.when(index < members - 1)
        def _():
            part_copy(index).start()

    def gather_rest():
        for hop in range(3, chain):
            to_other_core(hop)
        for hop in range(chain):
            for direction in (0, 1):
                if hop == 0 and direction == 1:
                    continue

                @pl.when(hop_arrives(hop, direction))
                def _():
                    shard = other - 2 * hop if direction == 0 else other + 2 * hop
                    remote(
                        wo_ref, out_w.at[shard], d_send.at[direction, hop],
                        d_recv.at[direction, hop], other, mine,
                    ).wait_recv()

        def load(src, shard):
            def one(index, carry):
                i, q = index // across, lax.rem(index, across)
                pltpu.make_async_copy(
                    src.at[
                        pl.ds(pl.multiple_of(i * LANES, LANES), LANES),
                        pl.ds(pl.multiple_of(q * LANES, LANES), LANES),
                    ],
                    held.at[at_shards + shard * shard_tiles + index],
                    load_sems.at[shard],
                ).start()
                return carry

            lax.fori_loop(0, shard_tiles, one, 0)

        def each(apart, carry):
            shard = lax.rem(dp + apart, dp_size)
            load(out_w.at[shard], shard)
            return carry

        def each_done(shard, carry):
            tiles = held.at[pl.ds(at_shards + shard * shard_tiles, shard_tiles)]
            pltpu.make_async_copy(tiles, tiles, load_sems.at[shard]).wait()
            return carry

        load(wo_ref, dp)
        lax.fori_loop(1, dp_size, each, 0)
        lax.fori_loop(0, dp_size, each_done, 0)

    lag_out = jnp.where(at_end, members - 1, 0)

    def finish_step(step, carry):
        @pl.when(step < members)
        def _():
            attend_block(step)

        @pl.when(step == lag_out)
        def _():
            gather_rest()

        @pl.when((step >= lag_out) & (step - lag_out < members))
        def _():
            project_block(step - lag_out)

        return carry

    lax.fori_loop(0, 2 * members - 1, finish_step, 0)

    def residual_wait(apart, carry):
        source = lax.rem(device + apart, devices)
        remote(
            x_ref.at[pl.ds(0, rows), :],
            residual.at[:, pl.ds(pl.multiple_of(source * lanes, lanes), lanes)],
            r_send.at[source], r_recv.at[source], other, mine,
        ).wait_recv()
        return carry

    lax.fori_loop(1, devices, residual_wait, 0)
    for apart in range(1, members):
        source = lax.rem(mine + apart, members)
        remote(
            held.at[pl.ds(at_own, model_tiles)],
            held.at[pl.ds(at_parts + source * model_tiles, model_tiles)], p_send.at[0], p_recv.at[source], dp, mine
        ).wait_recv()

    def add_up(piece, carry):
        span = pl.ds(pl.multiple_of(piece * LANES, LANES), LANES)
        summed = held[at_own + (members - 1) * model_tiles + piece].astype(f32)
        for apart in range(1, members):
            summed = summed + held[
                at_parts + lax.rem(mine + apart, members) * model_tiles + piece
            ].astype(f32)
        hidden_ref[:, span] = (residual[:, span].astype(f32) + summed).astype(bf16)
        return carry

    lax.fori_loop(0, model_tiles, add_up, 0, unroll=2)

    for copy in w_copies:
        copy.wait_send()

    def ids_sent(apart, carry):
        ids_copy(lax.rem(device + apart, devices)).wait_send()
        return carry

    lax.fori_loop(1, devices, ids_sent, 0)

    def features_sent(place_to, carry):
        def one(apart, inner):
            feature_copy(place_to, lax.rem(self_slot + apart, pool)).wait_send()
            return inner

        return lax.fori_loop(1, pool, one, carry)

    lax.fori_loop(0, chain, features_sent, 0)

    def passes_sent(index, carry):
        place_to = index // CHUNKS

        @pl.when(place_to != place)
        def _():
            passing_copy(0, place_to, lax.rem(index, CHUNKS)).wait_send()

        return carry

    lax.fori_loop(0, chain * CHUNKS, passes_sent, 0)
    for step in range(chain):

        @pl.when(step != place)
        def _():
            square_copy(step).wait_send()

    for hop in range(1, chain):
        for direction in (0, 1):

            @pl.when(hop_sends(hop, direction))
            def _():
                hop_copy(hop, direction).wait_send()

    for hop in range(chain):
        for direction in (0, 1):
            if hop == 0 and direction == 1:
                continue

            @pl.when(hop_arrives(hop, direction))
            def _():
                cross_copy(hop, direction, wo_ref).wait_send()

    def residual_sent(apart, carry):
        residual_copy(lax.rem(device + apart, devices)).wait_send()
        return carry

    lax.fori_loop(1, devices, residual_sent, 0)
    for index in range(members - 1):
        part_copy(index).wait_send()


def chain_call(lengths, ids, table, gain, cosine, sine, w_query, w_key, w_value, w_out):
    dp_size = lax.axis_size("dp")
    members = lax.axis_size("tensor")
    devices = dp_size * members
    chain = dp_size // 2
    pool = 2 * members
    rows = ids.shape[2]
    lanes, vocab = table.shape
    group_rows = rows * members
    depth = 2 * w_query.shape[0]
    q_width = w_query.shape[1]
    k_width = w_key.shape[1]
    model = lanes * devices
    bf16, f32 = jnp.bfloat16, jnp.float32
    dma = pltpu.SemaphoreType.DMA
    vmem = pl.BlockSpec(memory_space=pltpu.VMEM)
    hbm = pl.BlockSpec(memory_space=pl.ANY)
    return pl.pallas_call(
        chain_kernel,
        out_shape=(
            jax.ShapeDtypeStruct((rows, model), bf16),
            jax.ShapeDtypeStruct((1, 2, group_rows, k_width), bf16),
            jax.ShapeDtypeStruct((dp_size,) + w_out.shape, bf16),
        ),
        in_specs=[pl.BlockSpec(memory_space=pltpu.SMEM), vmem, hbm] + [vmem] * 6 + [hbm],
        out_specs=(vmem, vmem, hbm),
        scratch_shapes=[
            pltpu.VMEM((vocab // LANES, lanes, LANES), bf16),
            pltpu.VMEM((devices, 1, rows), jnp.int32),
            pltpu.SMEM((devices, 1, rows), jnp.int32),
            pltpu.VMEM((devices * rows, lanes), bf16),
            pltpu.VMEM((chain, group_rows, depth), bf16),
            pltpu.VMEM((depth, q_width), bf16),
            pltpu.VMEM((depth, 2 * k_width), bf16),
            pltpu.VMEM(w_query.shape, bf16),
            pltpu.VMEM(w_key.shape, bf16),
            pltpu.VMEM(w_value.shape, bf16),
            pltpu.VMEM((w_query.shape[0], HD), f32),
            pltpu.VMEM((2 * chain, 8, group_rows), f32),
            pltpu.VMEM((group_rows, HD), f32),
            pltpu.VMEM((rows, q_width), f32),
            pltpu.VMEM((chain - 1, CHUNKS, rows, q_width), bf16),
            pltpu.VMEM((chain + 1, CHUNKS, rows, q_width), bf16),
            pltpu.VMEM((rows, model), bf16),
            dma((1,)), dma((1,)), dma((devices,)), dma((devices,)),
            dma((3,)), dma((3,)),
            dma((chain * pool,)), dma((chain * pool,)),
            dma((chain,)), dma((chain,)),
            dma((chain * CHUNKS,)), dma((2, chain * CHUNKS)),
            dma((2, chain + 1)), dma((2, chain + 1)),
            dma((2, chain)), dma((2, chain)),
            dma((devices,)), dma((devices,)),
            dma((members,)), dma((members,)),
            dma((dp_size,)),
        ],
        compiler_params=pltpu.CompilerParams(has_side_effects=True, vmem_limit_bytes=67043328),
    )(lengths, ids, table, gain, cosine, sine, w_query, w_key, w_value, w_out)


def chain_shards(prompt_ids, prompt_lengths, embed_table, norm_gain, w_query, w_key, w_value, w_out):
    quarter = prompt_ids.shape[0]
    dp_size = lax.axis_size("dp")
    group_rows = quarter * lax.axis_size("tensor")
    half = HD // 2
    freq = np.float32(rope_theta) ** (-2.0 * np.arange(half, dtype=np.float32) / np.float32(HD))
    angle = np.arange(group_rows, dtype=np.float32)[:, None] * freq.astype(np.float32)[None, :]
    cosine = np.cos(angle.astype(np.float32))
    sine = np.sin(angle.astype(np.float32))
    hidden, cache, _ = chain_call(
        prompt_lengths, prompt_ids.reshape(1, 1, quarter), embed_table, norm_gain.reshape(dp_size, -1),
        jnp.asarray(np.concatenate([cosine, cosine], axis=1), jnp.float32),
        jnp.asarray(np.concatenate([-sine, sine], axis=1), jnp.float32),
        w_query, w_key, w_value, w_out,
    )
    return hidden, cache


def shards(prompt_ids, prompt_lengths, embed_table, *rest):
    members, dp_size = lax.axis_size("tensor"), lax.axis_size("dp")
    plain = members == TPG and dp_size % 2 == 0
    plain = plain and embed_table.shape[0] == LANES and prompt_ids.shape[0] == LANES
    return (chain_shards if plain else general_shards)(prompt_ids, prompt_lengths, embed_table, *rest)


def solution(mesh):
    in_specs = (
        P(("dp", "tensor")),
        P(),
        P(("dp", "tensor"), None),
        P(),
        P("dp", "tensor"),
        P("dp", "tensor"),
        P("dp", "tensor"),
        P("tensor", "dp"),
    )
    out_specs = (P(("dp", "tensor"), None), P(("dp", "tensor"), None, None, None))
    return jax.shard_map(shards, mesh=mesh, in_specs=in_specs, out_specs=out_specs, check_vma=False)
```

```python
import functools

import jax
import jax.numpy as jnp
import numpy as np
from jax import lax
from jax.experimental import pallas as pl
from jax.experimental.pallas import tpu as pltpu
from jax.sharding import PartitionSpec as P

HEADS = 32
KVH = 8
HD = 128
TPG = 4


norm_eps = 1e-05
rope_theta = 500000.0


def swapped(block, axis, apart):
    count = lax.axis_size(axis)
    route = []
    for low in range(count):
        high = low | 1 << apart
        if high != low and high < count:
            route += [(low, high), (high, low)]
    return lax.ppermute(block, axis, route)


def for_sending(shard):

    def short(part):
        return part.astype(jnp.bfloat16) if part.dtype == jnp.float32 else part

    return jax.tree.map(short, shard)


def rotate(heads_in, positions):
    half = heads_in.shape[-1] // 2
    freq = rope_theta ** (-2.0 * jnp.arange(half, dtype=jnp.float32) / heads_in.shape[-1])
    angle = positions.astype(jnp.float32)[:, None] * freq[None, :]
    cosine = jnp.cos(angle)[:, None, :]
    sine = jnp.sin(angle)[:, None, :]
    first = heads_in[..., :half]
    second = heads_in[..., half:]
    return jnp.concatenate(
        [first * cosine - second * sine, second * cosine + first * sine], axis=-1
    )


def attend(query_rot, key_rot, value_rows, length):
    row_count = query_rot.shape[0]
    block = min(512, row_count)
    positions = jnp.arange(row_count, dtype=jnp.int32)

    def one_block(offset):
        scores = jnp.einsum(
            "qhgd,khd->hgqk", query_rot, key_rot, preferred_element_type=jnp.float32
        ) / jnp.sqrt(jnp.float32(HD))
        query_pos = offset + jnp.arange(block, dtype=jnp.int32)
        allowed = (positions[None, :] <= query_pos[:, None]) & (positions[None, :] < length)
        scores = jnp.where(allowed, scores, -1e30)
        biggest = jnp.max(scores, axis=-1, keepdims=True)
        expd = jnp.exp(scores - biggest)
        weights = (expd / jnp.sum(expd, axis=-1, keepdims=True)).astype(jnp.bfloat16)
        result = jnp.einsum(
            "hgqk,khd->qhgd", weights, value_rows, preferred_element_type=jnp.float32
        )
        return result.astype(jnp.bfloat16)

    starts = jnp.arange(0, row_count, block, dtype=jnp.int32)
    outs = lax.map(one_block, starts)
    return outs.reshape(row_count, -1)


def ordered_pair(mine, theirs, bit_index, axis=0):
    upper_half = lax.axis_index("tensor") >> bit_index & 1 == 1
    first_half = jnp.where(upper_half, theirs, mine)
    second_half = jnp.where(upper_half, mine, theirs)
    return jnp.concatenate([first_half, second_half], axis=axis)


def collect_blocks(shard, swapper):
    stacked = shard[None]
    levels = lax.axis_size("tensor").bit_length() - 1
    for bit_index in range(TPG.bit_length() - 1, levels):
        stacked = ordered_pair(stacked, swapper(stacked, bit_index), bit_index)
    return stacked


def gather_in_group(own_part):
    bits = range(TPG.bit_length() - 1)
    width = own_part.shape[1] // len(bits)
    parts = [own_part[:, i * width : (i + 1) * width] for i in bits]
    axes = (1,) * len(bits)
    parts = [part.reshape(axes + part.shape) for part in parts]
    for step in bits:
        parts = [
            ordered_pair(
                part,
                swapped(part, "tensor", (i + step) % len(bits)),
                (i + step) % len(bits),
                len(bits) - 1 - (i + step) % len(bits),
            )
            for i, part in enumerate(parts)
        ]
    return jnp.concatenate([part.reshape(-1, width) for part in parts], axis=1)


def scatter_in_group(partial_sum):
    bits = range(TPG.bit_length() - 1)
    width = partial_sum.shape[1] // len(bits)
    rows = partial_sum.shape[0] // TPG
    shape = (2,) * len(bits) + (rows, width)
    parts = [partial_sum[:, i * width : (i + 1) * width].reshape(shape) for i in bits]
    for step in bits:
        moved = []
        for i, part in enumerate(parts):
            bit_index = (len(bits) - 1 - i - step) % len(bits)
            axis = len(bits) - 1 - bit_index
            lower = lax.slice_in_dim(part, 0, 1, axis=axis).astype(jnp.bfloat16)
            upper = lax.slice_in_dim(part, 1, 2, axis=axis).astype(jnp.bfloat16)
            upper_half = lax.axis_index("tensor") >> bit_index & 1 == 1
            kept = jnp.where(upper_half, upper, lower)
            given = jnp.where(upper_half, lower, upper)
            arrived = swapped(given, "tensor", bit_index)
            moved.append(kept.astype(jnp.float32) + arrived.astype(jnp.float32))
        parts = moved
    return jnp.concatenate([part.reshape(rows, width) for part in parts], axis=1)


def rms_normed(tokens_in, norm_gain):
    wide_in = tokens_in.astype(jnp.float32)
    scale = lax.rsqrt(jnp.mean(wide_in * wide_in, axis=1, keepdims=True) + norm_eps)
    return (wide_in * scale * norm_gain[None, :]).astype(jnp.bfloat16)


OUT_PARTS = 2
def exchange_kernel(per_target, block_ref, out_ref, own_sem, send_sems, recv_sems):
    width = lax.axis_size("tensor")
    count = lax.axis_size("dp") * width
    me = lax.axis_index("dp") * width + lax.axis_index("tensor")

    def copy_to(apart):
        target = lax.rem(me + apart, count)
        return pltpu.make_async_remote_copy(
            src_ref=block_ref.at[target] if per_target else block_ref.at[0],
            dst_ref=out_ref.at[me],
            send_sem=send_sems.at[apart],
            recv_sem=recv_sems.at[apart],
            device_id={"dp": target // width, "tensor": lax.rem(target, width)},
            device_id_type=pl.DeviceIdType.MESH,
        )

    def start(apart, carry):
        copy_to(apart).start()
        return carry

    def finish(apart, carry):
        copy_to(apart).wait()
        return carry

    own = pltpu.make_async_copy(
        block_ref.at[me] if per_target else block_ref.at[0], out_ref.at[me], own_sem
    )
    own.start()
    lax.fori_loop(1, count, start, 0)
    own.wait()
    lax.fori_loop(1, count, finish, 0)


def exchange(blocks, per_target):
    count = lax.axis_size(("dp", "tensor"))
    return pl.pallas_call(
        functools.partial(exchange_kernel, per_target),
        out_shape=jax.ShapeDtypeStruct((count,) + blocks.shape[1:], blocks.dtype),
        in_specs=[pl.BlockSpec(memory_space=pltpu.VMEM)],
        out_specs=pl.BlockSpec(memory_space=pltpu.VMEM),
        scratch_shapes=[
            pltpu.SemaphoreType.DMA,
            pltpu.SemaphoreType.DMA((count,)),
            pltpu.SemaphoreType.DMA((count,)),
        ],
        compiler_params=pltpu.CompilerParams(
            has_side_effects=True, vmem_limit_bytes=16 << 20
        ),
    )(blocks)


LANES = 128
PIECES = 6


def lookup_kernel(ids_ref, table_ref, out_ref, held, sems):
    columns, vocab = table_ref.shape
    tiles = vocab // LANES
    edges = [i * tiles // PIECES * LANES for i in range(PIECES + 1)]
    copies = [
        pltpu.make_async_copy(
            table_ref.at[:, low:high], held.at[:, low:high], sems.at[i]
        )
        for i, (low, high) in enumerate(zip(edges[:-1], edges[1:]))
    ]
    for copy in copies:
        copy.start()
    for copy in copies:
        copy.wait()
    lane = lax.broadcasted_iota(jnp.int32, (columns, LANES), 1)

    def block(index, carry):
        first = pl.multiple_of(index * LANES, LANES)

        def one(j, total):
            token = ids_ref[first + j]
            start = pl.multiple_of((token >> 7) * LANES, LANES)
            tile = held[:, pl.ds(start, LANES)]
            turned = pltpu.roll(tile, (j - token) & (LANES - 1), 1)
            return jnp.where(lane == j, turned, total)

        total = lax.fori_loop(
            0, LANES, one, jnp.zeros((columns, LANES), out_ref.dtype), unroll=32
        )
        out_ref[pl.ds(first, LANES), :] = total.T
        return carry

    lax.fori_loop(0, out_ref.shape[0] // LANES, block, 0)


def lookup_rows(embed_table, token_ids):
    columns = embed_table.shape[0]
    return pl.pallas_call(
        lookup_kernel,
        out_shape=jax.ShapeDtypeStruct((token_ids.shape[0], columns), embed_table.dtype),
        in_specs=[
            pl.BlockSpec(memory_space=pltpu.SMEM),
            pl.BlockSpec(memory_space=pl.ANY),
        ],
        out_specs=pl.BlockSpec(memory_space=pltpu.VMEM),
        scratch_shapes=[
            pltpu.VMEM(embed_table.shape, embed_table.dtype),
            pltpu.SemaphoreType.DMA((PIECES,)),
        ],
        compiler_params=pltpu.CompilerParams(vmem_limit_bytes=48 << 20),
        cost_estimate=pl.CostEstimate(
            flops=0, bytes_accessed=2 * embed_table.size, transcendentals=0
        ),
    )(token_ids, embed_table)


def general_shards(prompt_ids, prompt_lengths, embed_table, norm_gain, w_query, w_key, w_value, w_out):
    quarter = prompt_ids.shape[0]
    row_count = quarter * TPG
    devices = lax.axis_size(("dp", "tensor"))
    columns = embed_table.shape[0]
    model_width = columns * devices
    group_index = (
        lax.axis_index("dp") * (lax.axis_size("tensor") // TPG) + lax.axis_index("tensor") // TPG
    )
    length = lax.dynamic_slice_in_dim(prompt_lengths, group_index, 1, 0)[0]
    all_ids = exchange(prompt_ids.reshape(1, 1, quarter), False).reshape(-1)
    picked = lookup_rows(embed_table, all_ids)
    outgoing = picked.reshape(devices, quarter, columns)
    arrived = exchange(outgoing, True)
    own_rows = arrived.transpose(1, 0, 2).reshape(quarter, model_width)
    normed = gather_in_group(rms_normed(own_rows, norm_gain))
    query_width = w_query.shape[1]
    key_width = w_key.shape[1]
    packed = jnp.concatenate([w_query, w_key, w_value], axis=1)
    stacked = collect_blocks(
        packed,
        lambda values, bit_index: jax.tree.map(
            lambda part, own: part.astype(own.dtype),
            swapped(for_sending(values), "tensor", bit_index),
            values,
        ),
    )
    projected = jnp.einsum(
        "rd,kdc->rkc",
        normed,
        lax.all_gather(stacked, "dp", axis=1, tiled=True),
        preferred_element_type=jnp.float32,
    )
    blocks = projected.shape[1]
    local_heads = blocks * query_width // HD
    local_kv = blocks * key_width // HD
    positions = jnp.arange(row_count, dtype=jnp.int32)
    query = projected[:, :, :query_width].reshape(row_count, local_heads, HD)
    key_raw = projected[:, :, query_width : query_width + key_width].reshape(
        row_count, local_kv, HD
    )
    value_raw = projected[:, :, query_width + key_width :].reshape(row_count, local_kv, HD)
    query_rot = rotate(query, positions).astype(jnp.bfloat16)
    key_rot = rotate(key_raw, positions).astype(jnp.bfloat16)
    value_rows = value_raw.astype(jnp.bfloat16)
    cache = jnp.stack(
        [key_rot.reshape(row_count, local_kv * HD), value_rows.reshape(row_count, local_kv * HD)],
        axis=0,
    )[None]
    attended = attend(
        query_rot.reshape(row_count, local_kv, HEADS // KVH, HD), key_rot, value_rows, length
    )
    attended = attended.reshape(row_count, blocks, query_width)
    out_blocks = collect_blocks(
        w_out,
        lambda values, bit_index: jax.tree.map(
            lambda part, own: part.astype(own.dtype),
            swapped(for_sending(values), "tensor", bit_index),
            values,
        ),
    )
    width = out_blocks.shape[2] // OUT_PARTS
    reduced = []
    for i in range(OUT_PARTS):
        piece = out_blocks[:, :, i * width : (i + 1) * width]
        partial_sum = jnp.einsum(
            "rkw,kwc->rc",
            attended,
            lax.all_gather(piece, "dp", axis=2, tiled=True),
            preferred_element_type=jnp.float32,
        )
        own_sum = scatter_in_group(partial_sum).reshape(quarter, -1, width)
        attended, own_sum = lax.optimization_barrier((attended, own_sum))
        reduced.append(own_sum)
    running = jnp.concatenate(reduced, axis=2).reshape(quarter, model_width)
    hidden = (own_rows.astype(jnp.float32) + running).astype(jnp.bfloat16)
    return (hidden, cache)


CHUNKS = 6
TURN = 16


def chain_kernel(
    lengths_ref, ids_ref, table_ref, gain_ref, cos_ref, sin_ref, wq_ref, wk_ref, wv_ref, wo_ref,
    hidden_ref, cache_ref, out_w,
    held, ids_all, ids_scalar, x_ref,
    feats, mixed_q, mixed_kv, peer_q, peer_k, peer_v, gained, squares, scales, total, passed, inbox, residual,
    table_sems, ids_sems, i_send, i_recv,
    w_send, w_recv, x_send, x_recv, sq_send, sq_recv, rs_send, rs_recv,
    o_send, o_recv, d_send, d_recv, r_send, r_recv, p_send, p_recv, load_sems,
):
    f32, bf16 = jnp.float32, jnp.bfloat16
    dp_size = lax.axis_size("dp")
    members = lax.axis_size("tensor")
    chain = dp_size // 2
    dp = lax.axis_index("dp")
    mine = lax.axis_index("tensor")
    place = dp // 2
    core = lax.rem(dp, 2)
    pool = 2 * members
    self_slot = core * members + mine
    device = dp * members + mine
    lanes = x_ref.shape[1]
    group_rows = feats.shape[1]
    rows = group_rows // members
    shard_rows = wq_ref.shape[0]
    key_width = wk_ref.shape[1]
    heads_kv = key_width // HD
    ratio = HEADS // KVH
    model = lanes * dp_size * members
    depth, columns = wo_ref.shape
    devices = dp_size * members
    q_width = wq_ref.shape[1]
    at_shards = 0
    across = columns // LANES
    shard_tiles = depth // LANES * across
    q_tiles = q_width // LANES
    model_tiles = model // LANES
    at_attended = at_shards + dp_size * shard_tiles
    at_own = at_attended + members * q_tiles
    at_parts = at_own + members * model_tiles
    mesh_ids = pl.DeviceIdType.MESH

    def to(dp_index, tensor_index):
        return {"dp": dp_index, "tensor": tensor_index}

    def remote(src, dst, send_sem, recv_sem, dp_index, tensor_index):
        return pltpu.make_async_remote_copy(
            src_ref=src, dst_ref=dst, send_sem=send_sem, recv_sem=recv_sem,
            device_id=to(dp_index, tensor_index), device_id_type=mesh_ids,
        )

    other = dp + 1 - 2 * core

    w_copies = [
        remote(src, dst, w_send.at[i], w_recv.at[i], other, mine)
        for i, (src, dst) in enumerate(((wq_ref, peer_q), (wk_ref, peer_k), (wv_ref, peer_v)))
    ]
    for copy in w_copies:
        copy.start()

    def ids_copy(target):
        return remote(
            ids_ref.at[0], ids_all.at[device], i_send.at[target], i_recv.at[device],
            target // members, lax.rem(target, members),
        )

    def start_ids(apart, carry):
        ids_copy(lax.rem(device + apart, devices)).start()
        return carry

    lax.fori_loop(1, devices, start_ids, 0)
    ids_all[device] = ids_ref[0]

    def start_tile(tile, carry):
        pltpu.make_async_copy(
            table_ref.at[:, pl.ds(pl.multiple_of(tile * LANES, LANES), LANES)], held.at[tile], table_sems.at[0]
        ).start()
        return carry

    lax.fori_loop(0, held.shape[0], start_tile, 0, unroll=6)

    def wait_ids(apart, carry):
        source = lax.rem(device + apart, devices)
        remote(
            ids_ref.at[0], ids_all.at[source], i_send.at[source], i_recv.at[source], other, mine
        ).wait_recv()
        return carry

    lax.fori_loop(1, devices, wait_ids, 0)
    ids_copy_in = pltpu.make_async_copy(ids_all, ids_scalar, ids_sems.at[0])
    ids_copy_in.start()

    def feature_copy(place_to, slot):
        core_to = slot // members
        first = pl.multiple_of((2 * place_to + core_to) * group_rows, group_rows)
        return remote(
            x_ref.at[pl.ds(first, group_rows), :],
            feats.at[place_to, :, pl.ds(pl.multiple_of(self_slot * lanes, lanes), lanes)],
            x_send.at[place_to * pool + slot],
            x_recv.at[place_to * pool + self_slot],
            2 * place + core_to,
            lax.rem(slot, members),
        )

    lane = lax.broadcasted_iota(jnp.int32, (lanes, LANES), 1)
    turn_row = lax.broadcasted_iota(jnp.int32, (TURN, 2 * LANES), 0)
    turn_spot = lax.broadcasted_iota(jnp.int32, (TURN, 2 * LANES), 1)
    low_half = lax.broadcasted_iota(jnp.int32, (TURN, LANES), 0) % 4 < 2

    def tile_of(token):
        return held[token // LANES]

    def lookup_pair(pair, carry):
        first = pl.multiple_of(pair * 2 * LANES, LANES)
        second = pl.multiple_of(first + LANES, LANES)

        def turn(step, rolled):
            picked = jnp.zeros((TURN, 2 * LANES), f32)
            for four in range(0, TURN, 4):
                tokens = [ids_scalar[2 * pair + 1, 0, step * TURN + four + i] for i in range(4)]
                tiles_of = [tile_of(token) for token in tokens]
                where = jnp.full((TURN, 2 * LANES), -1, jnp.int32)
                for i, token in enumerate(tokens):
                    where = jnp.where(
                        turn_row == four + i, (token & (LANES - 1)) + (i % 2) * LANES, where
                    )
                chosen = jnp.where(where == turn_spot, 1.0, 0.0).astype(bf16)
                stacked = jnp.concatenate(
                    [jnp.concatenate(tiles_of[:2], axis=1), jnp.concatenate(tiles_of[2:], axis=1)],
                    axis=0,
                )
                picked = picked + lax.dot_general(
                    chosen, stacked, (((1,), (1,)), ((), ())), preferred_element_type=f32
                )
            x_ref[pl.ds(pl.multiple_of(second + step * TURN, TURN), TURN), :] = jnp.where(
                low_half, picked[:, :LANES], picked[:, LANES:]
            ).astype(bf16)
            for i in range(TURN):
                j = step * TURN + i
                token = ids_scalar[2 * pair, 0, j]
                turned = pltpu.roll(tile_of(token), (j - token) & (LANES - 1), 1)
                rolled = jnp.where(lane == j, turned, rolled)
            return rolled

        rolled = lax.fori_loop(0, LANES // TURN, turn, jnp.zeros((lanes, LANES), bf16), unroll=4)
        x_ref[pl.ds(first, LANES), :] = rolled.T
        return carry

    def order_of(index):
        found, picked = jnp.int32(0), jnp.int32(0)
        for step in range(chain - 1):
            for candidate, valid in (
                (chain - 1 - step, (chain - 1 - step > place).astype(jnp.int32)),
                (step, (step < place).astype(jnp.int32)),
            ):
                picked = picked + jnp.where((valid == 1) & (found == index), candidate, 0)
                found = found + valid
        return picked + jnp.where(index == chain - 1, place, 0)

    pairs = group_rows // (2 * LANES)

    def look_up(index, carry):
        place_to = order_of(index)

        def send(core_to):
            def one(apart, inner):
                slot = core_to * members + lax.rem(mine + apart, members)

                @pl.when(slot != self_slot)
                def _():
                    feature_copy(place_to, slot).start()

                return inner

            lax.fori_loop(1, members + 1, one, 0)

        def one_group(core_to, inner):
            group = 2 * place_to + core_to
            lax.fori_loop(group * pairs, (group + 1) * pairs, lookup_pair, 0)

            @pl.when(index < chain - 1)
            def _():
                send(core_to)

            @pl.when((index == chain - 1) & (core_to == 1))
            def _():
                send(0)
                send(1)

            @pl.when(core_to == core)
            def _():
                first = pl.multiple_of(group * group_rows, group_rows)
                feats[place_to, :, pl.ds(pl.multiple_of(self_slot * lanes, lanes), lanes)] = x_ref[
                    pl.ds(first, group_rows), :
                ]

            return inner

        lax.fori_loop(0, 2, one_group, 0)
        return carry

    def hop_copy(hop, direction):
        shard = dp - 2 * (hop - 1) if direction == 0 else dp + 2 * (hop - 1)
        target = dp + 2 if direction == 0 else dp - 2
        src = wo_ref if hop == 1 else out_w.at[shard]
        return remote(
            src, out_w.at[shard], o_send.at[direction, hop], o_recv.at[direction, hop], target, mine
        )

    def hop_sends(hop, direction):
        if direction == 0:
            return (place - (hop - 1) >= 0) & (place + 1 < chain)
        return (place + (hop - 1) < chain) & (place - 1 >= 0)

    def hop_arrives(hop, direction):
        return place - hop >= 0 if direction == 0 else place + hop < chain

    def hop_wait(hop, direction):
        shard = dp - 2 * hop if direction == 0 else dp + 2 * hop
        remote(
            wo_ref, out_w.at[shard], o_send.at[direction, hop], o_recv.at[direction, hop], other, mine
        ).wait_recv()

    def cross_copy(hop, direction, src):
        shard = dp - 2 * hop if direction == 0 else dp + 2 * hop
        return remote(
            src, out_w.at[shard], d_send.at[direction, hop], d_recv.at[direction, hop], other, mine
        )

    for direction in (0, 1):

        @pl.when(hop_sends(1, direction))
        def _():
            hop_copy(1, direction).start()

    cross_copy(0, 0, wo_ref).start()

    def gain_rows(core_of, q_ref, k_ref, v_ref):
        line = gain_ref[pl.ds(2 * place + core_of, 1), :]
        gained[...] = jnp.broadcast_to(line, (HD, shard_rows)).T
        first = pl.multiple_of(core_of * shard_rows, shard_rows)
        for src, dst, start in ((q_ref, mixed_q, 0), (k_ref, mixed_kv, 0), (v_ref, mixed_kv, key_width)):
            for low in range(0, src.shape[1], HD):
                dst[pl.ds(first, shard_rows), start + low : start + low + HD] = (
                    src[:, low : low + HD].astype(f32) * gained[...]
                ).astype(bf16)

    gain_rows(core, wq_ref, wk_ref, wv_ref)
    for copy in w_copies:
        copy.wait_recv()
    gain_rows(1 - core, peer_q, peer_k, peer_v)
    ids_copy_in.wait()
    pltpu.make_async_copy(held, held, table_sems.at[0]).wait()

    def square_copy(place_to):
        return remote(
            squares.at[chain + place_to], squares.at[place],
            sq_send.at[place_to], sq_recv.at[place], 2 * place_to + core, mine,
        )

    def features_ready(place_of):
        def one(apart, carry):
            slot = lax.rem(self_slot + apart, pool)
            remote(
                x_ref.at[pl.ds(0, group_rows), :],
                feats.at[place_of, :, pl.ds(pl.multiple_of(slot * lanes, lanes), lanes)],
                x_send.at[place_of * pool + slot],
                x_recv.at[place_of * pool + slot],
                other, mine,
            ).wait_recv()
            return carry

        lax.fori_loop(1, pool, one, 0)
        summed = jnp.zeros((group_rows, lanes), f32)
        for low in range(0, pool * lanes, lanes):
            wide = feats[place_of, :, low : low + lanes].astype(f32)
            summed = summed + wide * wide
        line = jnp.sum(summed.T, axis=0, keepdims=True)
        squares[chain + place_of] = jnp.broadcast_to(line, squares.shape[1:])

    def own_partial(place_of, chunk):
        @pl.when(chunk < 2)
        def _():
            for half in (0, 1):
                first = pl.multiple_of((2 * chunk + half) * rows, rows)
                total[:, half * 2 * key_width : (half + 1) * 2 * key_width] = jnp.dot(
                    feats[place_of, pl.ds(first, rows), :], mixed_kv[...], preferred_element_type=f32
                )

        @pl.when(chunk >= 2)
        def _():
            block = lax.rem(mine + chunk - 1, members)
            total[...] = jnp.dot(
                feats[place_of, pl.ds(pl.multiple_of(block * rows, rows), rows), :],
                mixed_q[...], preferred_element_type=f32,
            )

    def out_slot(place_to):
        return place_to - (place_to > place).astype(jnp.int32)

    def passing_copy(direction, place_to, chunk):
        return remote(
            passed.at[out_slot(place_to), chunk], inbox.at[place_to + 1 - direction, chunk],
            rs_send.at[place_to * CHUNKS + chunk], rs_recv.at[direction, place_to * CHUNKS + chunk],
            dp + 2 - 4 * direction, mine,
        )

    def from_side(direction, place_to, chunk):
        remote(
            passed.at[0, chunk], inbox.at[place_to + 1 - direction, chunk],
            rs_send.at[0], rs_recv.at[direction, place_to * CHUNKS + chunk], other, mine,
        ).wait_recv()
        total[...] += inbox[place_to + 1 - direction, chunk].astype(f32)

    lag_right = 2 * jnp.maximum(place - 1, 0)
    lag_left = 2 * jnp.maximum(chain - 2 - place, 0)
    right_count = CHUNKS * (chain - 1 - place)
    left_count = CHUNKS * place

    def pass_step(step, carry):
        direction = lax.rem(step, 2)
        index = step // 2 - jnp.where(direction == 0, lag_right, lag_left)
        count = jnp.where(direction == 0, right_count, left_count)

        @pl.when((index >= 0) & (index < count))
        def _():
            turn = index // CHUNKS
            chunk = lax.rem(index, CHUNKS)
            place_to = jnp.where(direction == 0, chain - 1 - turn, turn)

            @pl.when(chunk == 0)
            def _():
                features_ready(place_to)
                square_copy(place_to).start()

            own_partial(place_to, chunk)
            inner = jnp.where(direction == 0, place > 0, place < chain - 1)

            @pl.when(inner)
            def _():
                from_side(direction, place_to, chunk)

            passed[out_slot(place_to), chunk] = total[...].astype(bf16)
            passing_copy(direction, place_to, chunk).start()

        return carry

    at_end = (place == 0) | (place == chain - 1)

    def looked_up(turn):
        early = jnp.minimum(2 + turn // CHUNKS, chain)
        return jnp.where(turn < 0, 0, jnp.where(at_end, early, chain))

    def stream_turn(turn, carry):
        lax.fori_loop(looked_up(turn - 1), looked_up(turn), look_up, 0)
        for hop in range(2, chain):
            for direction in (0, 1):

                @pl.when((turn == CHUNKS * (hop - 2)) & hop_sends(hop, direction))
                def _():
                    hop_wait(hop - 1, direction)
                    hop_copy(hop, direction).start()

        return lax.fori_loop(2 * turn, 2 * turn + 2, pass_step, carry)

    lax.fori_loop(0, CHUNKS * (chain - 1) + 2 * max(chain - 2, 0), stream_turn, 0)

    def residual_copy(target):
        first = pl.multiple_of(target * rows, rows)
        return remote(
            x_ref.at[pl.ds(first, rows), :],
            residual.at[:, pl.ds(pl.multiple_of(device * lanes, lanes), lanes)],
            r_send.at[target], r_recv.at[device],
            target // members, lax.rem(target, members),
        )

    def start_residual(apart, carry):
        residual_copy(lax.rem(device + apart, devices)).start()
        return carry

    lax.fori_loop(1, devices, start_residual, 0)
    residual[:, pl.ds(pl.multiple_of(device * lanes, lanes), lanes)] = x_ref[
        pl.ds(pl.multiple_of(device * rows, rows), rows), :
    ]

    def to_other_core(hop):
        for direction in (0, 1):

            @pl.when(hop_arrives(hop, direction))
            def _():
                @pl.when(jnp.logical_not(hop_sends(hop + 1, direction)))
                def _():
                    hop_wait(hop, direction)

                shard = dp - 2 * hop if direction == 0 else dp + 2 * hop
                cross_copy(hop, direction, out_w.at[shard]).start()

    for hop in range(1, min(chain, 3)):
        to_other_core(hop)

    features_ready(place)
    squares[place] = squares[chain + place]
    for step in range(chain):

        @pl.when(step != place)
        def _():
            remote(
                squares.at[chain + step], squares.at[step],
                sq_send.at[step], sq_recv.at[step], other, mine,
            ).wait_recv()

    summed = squares[0]
    for step in range(1, chain):
        summed = summed + squares[step]
    line = lax.rsqrt(summed[0:1, :] * (1.0 / model) + norm_eps)
    scales[...] = jnp.broadcast_to(line, (HD, group_rows)).T

    def rotated(values, first):
        cosine = cos_ref[pl.ds(first, rows), :]
        sine = sin_ref[pl.ds(first, rows), :]
        return values * cosine + pltpu.roll(values, HD // 2, 1) * sine

    def finish_sum(chunk):
        own_partial(place, chunk)

        @pl.when(place > 0)
        def _():
            from_side(0, place, chunk)

        @pl.when(place < chain - 1)
        def _():
            from_side(1, place, chunk)

    def finish_kv(chunk, carry):
        finish_sum(chunk)
        for half in (0, 1):
            first = pl.multiple_of((2 * chunk + half) * rows, rows)
            scale = scales[pl.ds(first, rows), :]
            for head in range(heads_kv):
                low = half * 2 * key_width + head * HD
                key = rotated(total[:, low : low + HD] * scale, first)
                cache_ref[0, 0, pl.ds(first, rows), head * HD : (head + 1) * HD] = key.astype(bf16)
                value = total[:, low + key_width : low + key_width + HD] * scale
                cache_ref[0, 1, pl.ds(first, rows), head * HD : (head + 1) * HD] = value.astype(bf16)
        return carry

    lax.fori_loop(0, 2, finish_kv, 0)
    length = lengths_ref[dp]

    def attend_block(index):
        block = lax.rem(mine + 1 + index, members)
        first = pl.multiple_of(block * rows, rows)
        finish_sum(index + 2)
        scale = scales[pl.ds(first, rows), :]
        query_pos = first + lax.rem(
            lax.broadcasted_iota(jnp.int32, (ratio * rows, group_rows), 0), rows
        )
        key_pos = lax.broadcasted_iota(jnp.int32, (ratio * rows, group_rows), 1)
        allowed = (key_pos <= query_pos) & (key_pos < length)
        for head in range(heads_kv):
            queries = jnp.concatenate(
                [
                    rotated(total[:, low : low + HD] * scale, first).astype(bf16)
                    for low in range(head * ratio * HD, (head + 1) * ratio * HD, HD)
                ],
                axis=0,
            )
            keys = cache_ref[0, 0, :, head * HD : (head + 1) * HD]
            scores = lax.dot_general(
                queries, keys, (((1,), (1,)), ((), ())), preferred_element_type=f32
            ) * (HD ** -0.5)
            scores = jnp.where(allowed, scores, -1e30)
            expd = jnp.exp(scores - jnp.max(scores, axis=1, keepdims=True))
            weights = (expd / jnp.sum(expd, axis=1, keepdims=True)).astype(bf16)
            result = jnp.dot(
                weights, cache_ref[0, 1, :, head * HD : (head + 1) * HD], preferred_element_type=f32
            )
            for i in range(ratio):
                low = (head * ratio + i) * HD
                held[at_attended + index * q_tiles + head * ratio + i] = result[i * rows : (i + 1) * rows, :].astype(bf16)

    def part_copy(index):
        block = lax.rem(mine + 1 + index, members)
        return remote(
            held.at[pl.ds(at_own + index * model_tiles, model_tiles)],
            held.at[pl.ds(at_parts + mine * model_tiles, model_tiles)], p_send.at[index], p_recv.at[mine], dp, block
        )

    def project_block(index):
        def one(shard, carry):
            base = at_shards + shard * shard_tiles
            weights = jnp.concatenate(
                [
                    jnp.concatenate([held[base + i * across + q] for q in range(across)], axis=1)
                    for i in range(depth // LANES)
                ],
                axis=0,
            )
            heads = jnp.concatenate(
                [held[at_attended + index * q_tiles + head] for head in range(q_tiles)], axis=1
            )
            result = jnp.dot(heads, weights, preferred_element_type=f32).astype(bf16)
            for q in range(across):
                held[at_own + index * model_tiles + shard * across + q] = result[
                    :, q * LANES : (q + 1) * LANES
                ]
            return carry

        lax.fori_loop(0, dp_size, one, 0)

        @pl.when(index < members - 1)
        def _():
            part_copy(index).start()

    def gather_rest():
        for hop in range(3, chain):
            to_other_core(hop)
        for hop in range(chain):
            for direction in (0, 1):
                if hop == 0 and direction == 1:
                    continue

                @pl.when(hop_arrives(hop, direction))
                def _():
                    shard = other - 2 * hop if direction == 0 else other + 2 * hop
                    remote(
                        wo_ref, out_w.at[shard], d_send.at[direction, hop],
                        d_recv.at[direction, hop], other, mine,
                    ).wait_recv()

        def load(src, shard):
            def one(index, carry):
                i, q = index // across, lax.rem(index, across)
                pltpu.make_async_copy(
                    src.at[
                        pl.ds(pl.multiple_of(i * LANES, LANES), LANES),
                        pl.ds(pl.multiple_of(q * LANES, LANES), LANES),
                    ],
                    held.at[at_shards + shard * shard_tiles + index],
                    load_sems.at[shard],
                ).start()
                return carry

            lax.fori_loop(0, shard_tiles, one, 0)

        def each(apart, carry):
            shard = lax.rem(dp + apart, dp_size)
            load(out_w.at[shard], shard)
            return carry

        def each_done(shard, carry):
            tiles = held.at[pl.ds(at_shards + shard * shard_tiles, shard_tiles)]
            pltpu.make_async_copy(tiles, tiles, load_sems.at[shard]).wait()
            return carry

        load(wo_ref, dp)
        lax.fori_loop(1, dp_size, each, 0)
        lax.fori_loop(0, dp_size, each_done, 0)

    def finish_step(step, carry):
        attend_block(step)

        @pl.when(step == 0)
        def _():
            gather_rest()

        project_block(step)
        return carry

    lax.fori_loop(0, members, finish_step, 0)

    def residual_wait(apart, carry):
        source = lax.rem(device + apart, devices)
        remote(
            x_ref.at[pl.ds(0, rows), :],
            residual.at[:, pl.ds(pl.multiple_of(source * lanes, lanes), lanes)],
            r_send.at[source], r_recv.at[source], other, mine,
        ).wait_recv()
        return carry

    lax.fori_loop(1, devices, residual_wait, 0)
    for apart in range(1, members):
        source = lax.rem(mine + apart, members)
        remote(
            held.at[pl.ds(at_own, model_tiles)],
            held.at[pl.ds(at_parts + source * model_tiles, model_tiles)], p_send.at[0], p_recv.at[source], dp, mine
        ).wait_recv()

    def add_up(piece, carry):
        span = pl.ds(pl.multiple_of(piece * LANES, LANES), LANES)
        summed = held[at_own + (members - 1) * model_tiles + piece].astype(f32)
        for apart in range(1, members):
            summed = summed + held[
                at_parts + lax.rem(mine + apart, members) * model_tiles + piece
            ].astype(f32)
        hidden_ref[:, span] = (residual[:, span].astype(f32) + summed).astype(bf16)
        return carry

    lax.fori_loop(0, model_tiles, add_up, 0, unroll=2)

    for copy in w_copies:
        copy.wait_send()

    def ids_sent(apart, carry):
        ids_copy(lax.rem(device + apart, devices)).wait_send()
        return carry

    lax.fori_loop(1, devices, ids_sent, 0)

    def features_sent(place_to, carry):
        def one(apart, inner):
            feature_copy(place_to, lax.rem(self_slot + apart, pool)).wait_send()
            return inner

        return lax.fori_loop(1, pool, one, carry)

    lax.fori_loop(0, chain, features_sent, 0)

    def passes_sent(index, carry):
        place_to = index // CHUNKS

        @pl.when(place_to != place)
        def _():
            passing_copy(0, place_to, lax.rem(index, CHUNKS)).wait_send()

        return carry

    lax.fori_loop(0, chain * CHUNKS, passes_sent, 0)
    for step in range(chain):

        @pl.when(step != place)
        def _():
            square_copy(step).wait_send()

    for hop in range(1, chain):
        for direction in (0, 1):

            @pl.when(hop_sends(hop, direction))
            def _():
                hop_copy(hop, direction).wait_send()

    for hop in range(chain):
        for direction in (0, 1):
            if hop == 0 and direction == 1:
                continue

            @pl.when(hop_arrives(hop, direction))
            def _():
                cross_copy(hop, direction, wo_ref).wait_send()

    def residual_sent(apart, carry):
        residual_copy(lax.rem(device + apart, devices)).wait_send()
        return carry

    lax.fori_loop(1, devices, residual_sent, 0)
    for index in range(members - 1):
        part_copy(index).wait_send()


def chain_call(lengths, ids, table, gain, cosine, sine, w_query, w_key, w_value, w_out):
    dp_size = lax.axis_size("dp")
    members = lax.axis_size("tensor")
    devices = dp_size * members
    chain = dp_size // 2
    pool = 2 * members
    rows = ids.shape[2]
    lanes, vocab = table.shape
    group_rows = rows * members
    depth = 2 * w_query.shape[0]
    q_width = w_query.shape[1]
    k_width = w_key.shape[1]
    model = lanes * devices
    bf16, f32 = jnp.bfloat16, jnp.float32
    dma = pltpu.SemaphoreType.DMA
    vmem = pl.BlockSpec(memory_space=pltpu.VMEM)
    hbm = pl.BlockSpec(memory_space=pl.ANY)
    return pl.pallas_call(
        chain_kernel,
        out_shape=(
            jax.ShapeDtypeStruct((rows, model), bf16),
            jax.ShapeDtypeStruct((1, 2, group_rows, k_width), bf16),
            jax.ShapeDtypeStruct((dp_size,) + w_out.shape, bf16),
        ),
        in_specs=[pl.BlockSpec(memory_space=pltpu.SMEM), vmem, hbm] + [vmem] * 6 + [hbm],
        out_specs=(vmem, vmem, hbm),
        scratch_shapes=[
            pltpu.VMEM((vocab // LANES, lanes, LANES), bf16),
            pltpu.VMEM((devices, 1, rows), jnp.int32),
            pltpu.SMEM((devices, 1, rows), jnp.int32),
            pltpu.VMEM((devices * rows, lanes), bf16),
            pltpu.VMEM((chain, group_rows, depth), bf16),
            pltpu.VMEM((depth, q_width), bf16),
            pltpu.VMEM((depth, 2 * k_width), bf16),
            pltpu.VMEM(w_query.shape, bf16),
            pltpu.VMEM(w_key.shape, bf16),
            pltpu.VMEM(w_value.shape, bf16),
            pltpu.VMEM((w_query.shape[0], HD), f32),
            pltpu.VMEM((2 * chain, 8, group_rows), f32),
            pltpu.VMEM((group_rows, HD), f32),
            pltpu.VMEM((rows, q_width), f32),
            pltpu.VMEM((chain - 1, CHUNKS, rows, q_width), bf16),
            pltpu.VMEM((chain + 1, CHUNKS, rows, q_width), bf16),
            pltpu.VMEM((rows, model), bf16),
            dma((1,)), dma((1,)), dma((devices,)), dma((devices,)),
            dma((3,)), dma((3,)),
            dma((chain * pool,)), dma((chain * pool,)),
            dma((chain,)), dma((chain,)),
            dma((chain * CHUNKS,)), dma((2, chain * CHUNKS)),
            dma((2, chain + 1)), dma((2, chain + 1)),
            dma((2, chain)), dma((2, chain)),
            dma((devices,)), dma((devices,)),
            dma((members,)), dma((members,)),
            dma((dp_size,)),
        ],
        compiler_params=pltpu.CompilerParams(has_side_effects=True, vmem_limit_bytes=67043328),
    )(lengths, ids, table, gain, cosine, sine, w_query, w_key, w_value, w_out)


def chain_shards(prompt_ids, prompt_lengths, embed_table, norm_gain, w_query, w_key, w_value, w_out):
    quarter = prompt_ids.shape[0]
    dp_size = lax.axis_size("dp")
    group_rows = quarter * lax.axis_size("tensor")
    half = HD // 2
    freq = np.float32(rope_theta) ** (-2.0 * np.arange(half, dtype=np.float32) / np.float32(HD))
    angle = np.arange(group_rows, dtype=np.float32)[:, None] * freq.astype(np.float32)[None, :]
    cosine = np.cos(angle.astype(np.float32))
    sine = np.sin(angle.astype(np.float32))
    hidden, cache, _ = chain_call(
        prompt_lengths, prompt_ids.reshape(1, 1, quarter), embed_table, norm_gain.reshape(dp_size, -1),
        jnp.asarray(np.concatenate([cosine, cosine], axis=1), jnp.float32),
        jnp.asarray(np.concatenate([-sine, sine], axis=1), jnp.float32),
        w_query, w_key, w_value, w_out,
    )
    return hidden, cache


def shards(prompt_ids, prompt_lengths, embed_table, *rest):
    members, dp_size = lax.axis_size("tensor"), lax.axis_size("dp")
    plain = members == TPG and dp_size % 2 == 0
    plain = plain and embed_table.shape[0] == LANES and prompt_ids.shape[0] == LANES
    return (chain_shards if plain else general_shards)(prompt_ids, prompt_lengths, embed_table, *rest)


def solution(mesh):
    in_specs = (
        P(("dp", "tensor")),
        P(),
        P(("dp", "tensor"), None),
        P(),
        P("dp", "tensor"),
        P("dp", "tensor"),
        P("dp", "tensor"),
        P("tensor", "dp"),
    )
    out_specs = (P(("dp", "tensor"), None), P(("dp", "tensor"), None, None, None))
    return jax.shard_map(shards, mesh=mesh, in_specs=in_specs, out_specs=out_specs, check_vma=False)
```
